32 devices in a mesh: patch: 32 (over z, y, x, core).
Axes of the slice: x: 2, y: 2, z: 4, core: 2. Of those that a mesh axis runs over, the one named last changes fastest.
Arguments:
- positions: float32 [3, 65536], P(None, 'patch'), may hold values from -6 to 6
- densities: float32 [3, 65536], P(None, 'patch'), may hold values from -6 to 6
- near_src: int32 [512, 8], P('patch'), may hold values from 0 to 511, as said below
- near_count: int32 [512], P('patch'), may hold values from 1 to 8
- far_slot: int32 [512, 32], P('patch'), may hold values from 0 to 127
- far_class: int32 [512, 32], P('patch'), may hold values from 0 to 188
- far_count: int32 [512], P('patch'), may hold values from 1 to 32
- requests: int32 [32, 32, 4], P('patch'), may hold values from 0 to 15, as said below
- up_basis: bfloat16 [512, 144, 384], P('patch'), may hold values from -0.3125 to 0.3125
- transfer_table: bfloat16 [189, 20736], replicated, may hold values from -0.5 to 0.5
- down_basis: bfloat16 [512, 144, 9, 128], P('patch'), may hold values from -0.09375 to 0.09375
Outputs:
- shape_grad: float32 [3, 65536], P(None, 'patch')
The draws below stay inside these ranges and needn't reach their ends.
Inputs may be any that keep to these rules, and one draw needn't show every extreme that they name: `near_src`: the source leaf of each near-field block is held by the device of its target leaf or by the device just before or after it along patch. `requests`: each row names 4 different leaves of the source device, by their index on that device.
All inputs are finite; a program needn't handle non-finite values.
Results may differ from the reference program's by a relative error of at most 0.0042.
Values may be sent and summed in bfloat16 or wider, within the bound.
A program may use at most 192 MiB of HBM per device.

```python
import math
import jax
import jax.numpy as jnp
from jax import lax

P_SIZE = 128
RANK = 48
LEAF_DEV = 16
NEAR = 8
FAR = 32
CLASSES = 189
CAP = 4
LEAVES = 512
NODES = 65536
SLOTS = 128
N_PATCH = 32


def draw_near_src(key, part):
    leaves = jnp.arange(LEAVES, dtype=jnp.int32)
    owner = leaves // LEAF_DEV
    last_dev = LEAVES // LEAF_DEV - 1
    span = jnp.where((owner == 0) | (owner == last_dev), 2 * LEAF_DEV, 3 * LEAF_DEV)
    lowest = jnp.where(owner == 0, 0, (owner - 1) * LEAF_DEV)
    raw = jax.random.randint(jax.random.fold_in(key, 11), (LEAVES, NEAR), 0, 1 << 30)
    return (lowest[:, None] + raw % span[:, None]).astype(jnp.int32)


def draw_near_count(key, part):
    first, second, third = jax.random.split(jax.random.fold_in(key, 12), 3)
    ndev = LEAVES // LEAF_DEV
    level = jax.random.randint(first, (ndev,), max(1, NEAR // 4), NEAR + 1)
    raw = jax.random.randint(second, (LEAVES,), 0, 1 << 30)
    count = 1 + raw % jnp.repeat(level, LEAF_DEV)
    chosen = jax.random.randint(third, (), 0, ndev)
    leaves = jnp.arange(LEAVES, dtype=jnp.int32)
    return jnp.where(leaves == chosen * LEAF_DEV, NEAR, count).astype(jnp.int32)


def draw_requests(key, part):
    ndev = LEAVES // LEAF_DEV
    scores = jax.random.randint(jax.random.fold_in(key, 13), (ndev, ndev, LEAF_DEV), 0, 1 << 20)
    scores = scores * LEAF_DEV + jnp.arange(LEAF_DEV, dtype=jnp.int32)
    order = jnp.argsort(scores, axis=-1, stable=True)
    return order[:, :, :CAP].astype(jnp.int32)


def with_ends(entries, own_key, least, top_value):
    longest = entries.shape.index(max(entries.shape))
    spots = []
    for shift in (0, 1):
        where = [jax.random.randint(jax.random.fold_in(own_key, axis), (), 0, length) for axis, length in enumerate(entries.shape)]
        where[longest] = (where[longest] + shift) % entries.shape[longest]
        spots.append(tuple(where))
    return entries.at[spots[0]].set(least).at[spots[1]].set(top_value)


def steps_of(stream_key, shape, cuts, low, high):
    def one(position, blocks):
        draws = jax.random.uniform(jax.random.fold_in(jax.random.fold_in(stream_key, 6), position), (blocks,), jnp.float32, low / len(cuts), high / len(cuts))
        return jnp.repeat(jnp.exp(draws), shape[position] // blocks).reshape((-1,) + (1,) * (len(shape) - position - 1))

    factor_of = one(*cuts[0])
    for cut in cuts[1:]:
        factor_of = factor_of * one(*cut)
    return factor_of


def gaussian(own_key, extent, spread, most, pieces=(), kind=jnp.bfloat16):
    gain = steps_of(own_key, extent, pieces, -0.22, 0.18) if pieces else 1.0
    entries = jax.random.normal(own_key, extent, jnp.float32) * spread * gain
    return jnp.minimum(jnp.maximum(entries, -most), most).astype(kind)


def setup_inputs(seed: int = 0) -> dict:
    splits = jax.random.split(jax.random.key(seed), 12)
    positions = gaussian(splits[0], (3, NODES), 1.0, 6.0, ((1, 32),), jnp.float32)
    densities = gaussian(splits[1], (3, NODES), 1.0, 6.0, ((1, 32),), jnp.float32)
    near_src = draw_near_src(jax.random.fold_in(splits[11], 71), 0)
    near_count = draw_near_count(jax.random.fold_in(splits[11], 71), 0)
    far_slot = with_ends(jax.random.randint(splits[4], (LEAVES, FAR), 0, SLOTS), jax.random.fold_in(splits[4], 1), 0, SLOTS - 1).astype(jnp.int32)
    far_class = with_ends(jax.random.randint(splits[5], (LEAVES, FAR), 0, CLASSES), jax.random.fold_in(splits[5], 1), 0, CLASSES - 1).astype(jnp.int32)
    far_count = with_ends(jax.random.randint(splits[6], (LEAVES,), 1, FAR + 1), jax.random.fold_in(splits[6], 1), 1, FAR).astype(jnp.int32)
    requests = draw_requests(jax.random.fold_in(splits[11], 71), 0)
    up_basis = gaussian(splits[8], (LEAVES, 3 * RANK, 3 * P_SIZE), (3 * P_SIZE) ** -0.5, 0.3125, ((0, 32),))
    transfer_table = gaussian(splits[9], (CLASSES, 9 * RANK * RANK), (3 * RANK) ** -0.5, 0.5)
    down_basis = gaussian(splits[10], (LEAVES, 3 * RANK, 9, P_SIZE), (3 * RANK * FAR) ** -0.5, 0.09375, ((0, 32),))
    return dict(positions=positions, densities=densities, near_src=near_src, near_count=near_count, far_slot=far_slot, far_class=far_class, far_count=far_count, requests=requests, up_basis=up_basis, transfer_table=transfer_table, down_basis=down_basis)


KERNEL = 1.0 / (8.0 * math.pi)
BLOB = 0.25

def pair_terms(target, source):
    xt = target[:, :3]
    ft = target[:, 3:]
    xs = source[:, :3]
    fs = source[:, 3:]
    sep = xt[:, :, :, None] - xs[:, :, None, :]
    rho_sq = lax.optimization_barrier(jnp.sum(sep * sep, axis=1)) + BLOB
    inv_one = lax.rsqrt(rho_sq)
    inv_three = inv_one / rho_sq
    inv_five = inv_three / rho_sq
    fa = ft[:, :, :, None]
    fb = fs[:, :, None, :]
    prod_ab = lax.optimization_barrier(jnp.sum(fa * fb, axis=1))
    prod_ar = lax.optimization_barrier(jnp.sum(fa * sep, axis=1))
    prod_br = lax.optimization_barrier(jnp.sum(fb * sep, axis=1))
    first = (fa * prod_br[:, None] + fb * prod_ar[:, None] - prod_ab[:, None] * sep) * inv_three[:, None]
    second = 3.0 * (prod_ar * prod_br * inv_five)[:, None] * sep
    return (first - second) * KERNEL

def reference(positions, densities, near_src, near_count, far_slot, far_class, far_count, requests, up_basis, transfer_table, down_basis):
    stacked = jnp.concatenate([positions, densities], 0).reshape(6, LEAVES, P_SIZE).transpose(1, 0, 2)
    blocks = jnp.arange(N_PATCH, dtype=jnp.int32)

    def slot_body(slot, grad):
        source = near_src[:, slot]
        live = (slot < near_count).astype(jnp.float32)

        def one_block(block):
            start = (block * LEAF_DEV).astype(jnp.int32)
            target = lax.dynamic_slice_in_dim(stacked, start, LEAF_DEV, 0)
            src_ids = lax.dynamic_slice_in_dim(source, start, LEAF_DEV, 0)
            weight = lax.dynamic_slice_in_dim(live, start, LEAF_DEV, 0)
            terms = pair_terms(target, stacked[src_ids]) * weight[:, None, None, None]
            return (lax.optimization_barrier(jnp.sum(terms, axis=3)), lax.optimization_barrier(jnp.sum(terms, axis=2)))
        tgt_sum, src_sum = lax.map(one_block, blocks)
        grad = grad + tgt_sum.reshape(LEAVES, 3, P_SIZE)
        return grad.at[source].add(-src_sum.reshape(LEAVES, 3, P_SIZE))
    near = lax.fori_loop(0, NEAR, slot_body, jnp.zeros((LEAVES, 3, P_SIZE), jnp.float32))
    dens_leaf = stacked[:, 3:]
    dens_round = lax.optimization_barrier(dens_leaf.reshape(LEAVES, 3 * P_SIZE).astype(jnp.bfloat16))
    dens_flat = dens_round.astype(jnp.float32)

    def upward(block):
        start = (block * LEAF_DEV).astype(jnp.int32)
        basis = lax.dynamic_slice_in_dim(up_basis, start, LEAF_DEV, 0).astype(jnp.float32)
        dens_b = lax.dynamic_slice_in_dim(dens_flat, start, LEAF_DEV, 0)
        return jnp.einsum('lrq,lq->lr', basis, dens_b, precision=lax.Precision.HIGHEST).astype(jnp.bfloat16)
    moments = lax.map(upward, blocks).reshape(LEAVES, 3 * RANK)
    moments = lax.optimization_barrier(moments).astype(jnp.float32)
    dev_of = jnp.arange(LEAVES, dtype=jnp.int32) // LEAF_DEV
    peer = far_slot // CAP
    place = far_slot % CAP
    source_ids = peer * LEAF_DEV + requests[dev_of[:, None], peer, place]

    def far_block(block):
        start = (block * LEAF_DEV).astype(jnp.int32)
        ids = lax.dynamic_slice_in_dim(source_ids, start, LEAF_DEV, 0)
        classes = lax.dynamic_slice_in_dim(far_class, start, LEAF_DEV, 0)
        counts = lax.dynamic_slice_in_dim(far_count, start, LEAF_DEV, 0)

        def far_step(slot, expansion):
            src = moments[ids[:, slot]]
            oper = transfer_table[classes[:, slot]].reshape(LEAF_DEV, 3 * RANK, 3 * RANK).astype(jnp.float32)
            live = (slot < counts).astype(jnp.float32)
            return expansion + live[:, None] * jnp.einsum('lij,lj->li', oper, src, precision=lax.Precision.HIGHEST)
        expansion = lax.fori_loop(0, FAR, far_step, jnp.zeros((LEAF_DEV, 3 * RANK), jnp.float32))
        expansion = lax.optimization_barrier(expansion.astype(jnp.bfloat16)).astype(jnp.float32)
        basis = lax.dynamic_slice_in_dim(down_basis, start, LEAF_DEV, 0).astype(jnp.float32)
        field = jnp.einsum('lr,lrqp->lqp', expansion, basis, precision=lax.Precision.HIGHEST)
        dens_b = lax.dynamic_slice_in_dim(dens_leaf, start, LEAF_DEV, 0)
        return jnp.einsum('lcp,lckp->lkp', dens_b, field.reshape(LEAF_DEV, 3, 3, P_SIZE), precision=lax.Precision.HIGHEST)
    far = lax.map(far_block, blocks).reshape(LEAVES, 3, P_SIZE)
    return (near + far).transpose(1, 0, 2).reshape(3, NODES)
```

```python
import functools
import math

import jax
import jax.numpy as jnp
import numpy as np
from jax import lax
from jax.experimental import pallas as pl
from jax.experimental.pallas import tpu as pltpu
from jax.sharding import PartitionSpec as P

KERNEL = 1.0 / (8.0 * math.pi)
BLOB = 0.25
MESH = pl.DeviceIdType.MESH
F32 = jnp.float32
BF16 = jnp.bfloat16

ROWS = 48
FEATURES = 48
LEFT = (0, 0, 0, 1, 1, 2)
RIGHT = (0, 1, 2, 0, 1, 0)


def at(group):
    return (group // 2) * 8 + (group % 2) * 3


def source_choice():
    sel = np.zeros((4, FEATURES, ROWS), np.float32)
    for k in range(6):
        for c in range(3):
            sel[0, 3 * k + c, at(3 + RIGHT[k]) + c] = 1.0
            sel[1, 3 * k + c, at(6 + RIGHT[k]) + c] = -1.0
            sel[2, 18 + 3 * k + c, at(RIGHT[k]) + c] = 1.0
            sel[3, 18 + 3 * k + c, at(6 + RIGHT[k]) + c] = -2.0
    for c in range(3):
        sel[1, 36 + c, at(11) + c] = 1.0
        sel[2, 42 + c, at(9) + c] = -1.0
        sel[3, 39 + c, at(11) + c] = 1.0
        sel[3, 42 + c, at(10) + c] = 1.0
    return sel.reshape(4 * FEATURES, ROWS)


def target_choice(size):
    sel = np.zeros((ROWS, 128), np.float32)
    spread = np.zeros((ROWS, 6, size), np.float32)
    for k in range(6):
        for c in range(3):
            sel[at(LEFT[k]) + c, 3 * k + c] = 1.0
            sel[at(3 + LEFT[k]) + c, 18 + 3 * k + c] = 1.0
    for c in range(3):
        sel[at(6) + c, 36 + c] = 1.0
        sel[at(7) + c, 39 + c] = 1.0
        sel[at(8) + c, 42 + c] = 1.0
        for piece in range(3):
            spread[at(3 + piece) + c, c, :] = 3.0
            spread[at(piece) + c, 3 + c, :] = 1.0
    return np.concatenate([sel, spread.reshape(ROWS, 6 * size)], axis=1)


def iota(shape, dim):
    return lax.broadcasted_iota(jnp.int32, shape, dim)


def dot(a, b):
    return jnp.dot(a, b, preferred_element_type=F32)


def pieces(x):
    high = x.astype(BF16).astype(F32)
    rest = x - high
    mid = rest.astype(BF16).astype(F32)
    return high, mid, rest - mid


def inner(a, b):
    return a[0:1] * b[0:1] + a[1:2] * b[1:2] + a[2:3] * b[2:3]


def put(rows, group, value):
    rows[at(group) : at(group) + value.shape[0], : value.shape[1]] = value


def put_pieces(rows, group, value):
    for k, piece in enumerate(pieces(value)):
        if value.shape[0] == 3:
            put(rows, group + k, piece)
        else:
            rows[at(group) + k : at(group) + k + 1, : value.shape[1]] = piece


def source_rows(rows, x, f):
    put_pieces(rows, 0, f)
    put_pieces(rows, 3, f * (1.0 / 3.0))
    put_pieces(rows, 6, x)
    put_pieces(rows, 9, inner(f, x))
    put_pieces(rows, 10, inner(x, x) + BLOB)
    put(rows, 11, jnp.ones_like(x))


def target_rows(rows, x, f):
    a = f * KERNEL
    put_pieces(rows, 0, a)
    put_pieces(rows, 3, x)
    put_pieces(rows, 6, inner(a, x))
    put_pieces(rows, 7, inner(x, x))
    put(rows, 8, jnp.ones_like(x))


def flip(me, bit):
    return me + bit - 2 * bit * lax.rem(lax.div(me, bit), 2)


def body(
    n,
    near_src,
    near_count,
    far_count,
    pos,
    dens,
    far_slot,
    far_class,
    req,
    choose_src,
    choose_tgt,
    up_hbm,
    table_hbm,
    down_hbm,
    out,
    pos_b,
    pos_a,
    dens_b,
    dens_a,
    up,
    table,
    down,
    dens_rows,
    mom,
    rows_own,
    rows_oth,
    window,
    rhs,
    lhs,
    tb,
    geo0,
    geo1,
    tacc,
    cols,
    src_rows,
    hot_src,
    part_b,
    part_a,
    got_b,
    got_a,
    hot_class,
    hot_slot,
    tiled,
    sums,
    fold,
    expan,
    field,
    up_sem,
    table_sem,
    down_sem,
    halo_send,
    halo_recv,
    mom_send,
    mom_recv,
    part_send,
    part_recv,
):
    leaves, width = mom.shape[1:]
    nodes = pos.shape[1]
    size = nodes // leaves
    slots = near_src.shape[0]
    far_num = far_slot.shape[1]
    classes = table.shape[0]
    cap = req.shape[0]
    block = fold.shape[0]
    phases = n.bit_length() - 1
    me = lax.axis_index("patch")
    has_left = me > 0
    has_right = me < n - 1
    barrier = pltpu.get_barrier_semaphore()

    def signal(peer):
        pl.semaphore_signal(barrier, inc=1, device_id=(peer,), device_id_type=MESH)

    for t in range(phases):
        signal(flip(me, n >> (t + 1)))

    @pl.when(has_left)
    def _():
        signal(me - 1)

    @pl.when(has_right)
    def _():
        signal(me + 1)

    get_up = pltpu.make_async_copy(up_hbm, up, up_sem)
    get_up.start()

    def table_copy(b):
        lanes = pl.ds(pl.multiple_of(b * block, 128), block)
        return pltpu.make_async_copy(
            table_hbm.at[:, lanes], table.at[:, lanes], table_sem.at[b]
        )

    for b in range(width * width // block):
        table_copy(b).start()
    get_down = pltpu.make_async_copy(down_hbm, down, down_sem)
    get_down.start()

    for leaf in range(leaves):
        for c in range(3):
            dens_rows[leaf : leaf + 1, c * size : (c + 1) * size] = dens[
                c : c + 1, leaf * size : (leaf + 1) * size
            ]
    dens_round = dens_rows[...].astype(BF16)
    get_up.wait()
    row = iota((leaves, width), 0)
    total = jnp.zeros((leaves, width), F32)
    for leaf in range(leaves):
        got = lax.dot_general(
            dens_round, up[leaf], (((1,), (1,)), ((), ())), preferred_element_type=F32
        )
        total = total + jnp.where(row == leaf, got, 0.0)
    mom[0] = total.astype(BF16)

    def halo(k, src, dst, peer):
        return pltpu.make_async_remote_copy(
            src_ref=src,
            dst_ref=dst,
            send_sem=halo_send.at[k],
            recv_sem=halo_recv.at[k],
            device_id=(peer,),
            device_id_type=MESH,
        )

    to_right = (halo(0, pos, pos_b, me + 1), halo(1, dens, dens_b, me + 1))
    to_left = (halo(2, pos, pos_a, me - 1), halo(3, dens, dens_a, me - 1))

    def gather(t):
        return pltpu.make_async_remote_copy(
            src_ref=mom.at[0 : 1 << t],
            dst_ref=mom.at[1 << t : 2 << t],
            send_sem=mom_send.at[t],
            recv_sem=mom_recv.at[t],
            device_id=(flip(me, n >> (t + 1)),),
            device_id_type=MESH,
        )

    pl.semaphore_wait(
        barrier, phases + has_left.astype(jnp.int32) + has_right.astype(jnp.int32)
    )

    @pl.when(has_right)
    def _():
        for copy in to_right:
            copy.start()

    @pl.when(has_left)
    def _():
        for copy in to_left:
            copy.start()

    gather(0).start()

    rows_own[...] = jnp.zeros_like(rows_own)
    rows_oth[...] = jnp.zeros_like(rows_oth)
    target_rows(rows_own, pos[...], dens[...])

    @pl.loop(0, leaves)
    def _(leaf):
        lanes = pl.ds(pl.multiple_of(leaf * size, size), size)
        turned = jnp.transpose(rows_own[:, lanes]).astype(BF16)
        lhs[leaf] = dot(turned, choose_tgt[:, :128]).astype(BF16)
        tb[leaf] = dot(turned, choose_tgt[:, 128:])

    def sources(part, rows, x, f):
        source_rows(rows, x[...], f[...])
        for leaf in range(leaves):
            lanes = slice(leaf * size, (leaf + 1) * size)
            window[part * leaves + leaf, 0:3, :] = x[:, lanes] * 3.0
            window[part * leaves + leaf, 3:6, :] = f[:, lanes]

        @pl.loop(0, leaves)
        def _(leaf):
            lanes = pl.ds(pl.multiple_of(leaf * size, size), size)
            chosen = dot(choose_src[...], rows[:, lanes].astype(BF16)).astype(BF16)
            for o in range(4):
                rhs[part * leaves + leaf, :, o * size : (o + 1) * size] = chosen[
                    o * FEATURES : (o + 1) * FEATURES
                ]

    window[...] = jnp.zeros_like(window)
    nothing = jnp.zeros((3, size), F32)
    source_rows(rows_oth, nothing, nothing)
    chosen = dot(choose_src[...], rows_oth[:, :size].astype(BF16)).astype(BF16)
    for o in range(4):
        rhs[3 * leaves, :, o * size : (o + 1) * size] = chosen[
            o * FEATURES : (o + 1) * FEATURES
        ]
    sources(1, rows_oth, pos, dens)

    count_col = jnp.zeros((leaves, 1), jnp.int32)
    leaf_col = iota((leaves, 1), 0)
    for leaf in range(leaves):
        count_col = jnp.where(leaf_col == leaf, far_count[leaf], count_col)
    class_iota = iota((leaves, classes), 1)
    column = iota((leaves, cap * n), 1)
    slot_of = lax.rem(column, n) * cap + lax.div(column, n)
    for s in range(far_num):
        rows = slice(s * leaves, (s + 1) * leaves)
        wanted = jnp.where(s < count_col, far_class[:, s : s + 1], -1)
        hot_class[rows, :] = (class_iota == wanted).astype(F32).astype(BF16)
        slot = far_slot[:, s : s + 1]
        hot_slot[rows, :] = (slot_of == slot).astype(F32).astype(BF16)
    fold_row = iota(fold.shape, 0)
    fold_first = iota(fold.shape, 1) * width
    fold[...] = (
        ((fold_row >= fold_first) & (fold_row < fold_first + width)).astype(F32).astype(BF16)
    )
    cols[...] = jnp.zeros_like(cols)

    @pl.when(has_left)
    def _():
        for copy in to_right:
            copy.wait_recv()

    @pl.when(jnp.logical_not(has_left))
    def _():
        pos_b[...] = jnp.zeros_like(pos_b)
        dens_b[...] = jnp.zeros_like(dens_b)

    sources(0, rows_oth, pos_b, dens_b)

    @pl.when(has_right)
    def _():
        for copy in to_left:
            copy.wait_recv()

    @pl.when(jnp.logical_not(has_right))
    def _():
        pos_a[...] = jnp.zeros_like(pos_a)
        dens_a[...] = jnp.zeros_like(dens_a)

    sources(2, rows_own, pos_a, dens_a)

    offset = (me - 1) * leaves
    lane8 = iota((8, size), 1)
    lane1 = iota((1, 128), 1)

    def source_of(leaf, slot):
        live = slot < near_count[leaf]
        return jnp.where(live, near_src[slot, leaf] - offset, 3 * leaves)

    def geometry(geo, leaf, first):
        for k in range(2):
            geo[k] = dot(lhs[leaf][:, :FEATURES], rhs[source_of(leaf, first + k)])

    geometry(geo0, 0, 0)
    pairs = slots // 2

    @pl.loop(0, leaves)
    def _(leaf):
        for t in range(1, phases):
            @pl.when(leaf == ((t - 1) * leaves) // max(phases - 1, 1))
            def _():
                gather(t - 1).wait_recv()
                gather(t).start()

        following = lax.rem(leaf + 1, leaves)
        for pair in range(pairs):
            geo, other = ((geo0, geo1), (geo1, geo0))[pair % 2]
            if pair + 1 < pairs:
                geometry(other, leaf, 2 * pair + 2)
            else:
                geometry(other, following, 0)
            xs, fs, sums_src = [], [], []
            for k in range(2):
                index = source_of(leaf, 2 * pair + k)
                nodes_k = window[index]
                xs.append([jnp.broadcast_to(nodes_k[c : c + 1], (8, size)) for c in range(3)])
                fs.append([jnp.broadcast_to(nodes_k[3 + c : 4 + c], (8, size)) for c in range(3)])
                sums_src.append([None] * 3)
                hot_src[leaf, 2 * pair + k : 2 * pair + k + 1, :] = (lane1 == index).astype(F32)
            for g in range(size // 8):
                r8 = slice(g * 8, (g + 1) * 8)
                total = [None] * 3
                for k in range(2):
                    ab, ar, br, rho = [
                        geo[k, r8, o * size : (o + 1) * size] for o in range(4)
                    ]
                    inv1 = lax.rsqrt(rho)
                    inv2 = inv1 * inv1
                    inv3 = inv1 * inv2
                    p = br * inv3
                    q = ar * inv3
                    w = ab * inv3 + (p * ar) * inv2
                    for c in range(3):
                        sep = tb[leaf, r8, c * size : (c + 1) * size] - xs[k][c]
                        a = tb[leaf, r8, (3 + c) * size : (4 + c) * size]
                        term = a * p + fs[k][c] * q - w * sep
                        sums_src[k][c] = term if g == 0 else sums_src[k][c] + term
                        total[c] = term if k == 0 else total[c] + term
                for c in range(3):
                    if pair > 0:
                        total[c] = total[c] + tacc[c, r8, :]
                    if pair + 1 < pairs:
                        tacc[c, r8, :] = total[c]
                    else:
                        col = jnp.sum(total[c], axis=1, keepdims=True)
                        cols[r8, :] = jnp.where(lane8 == c * leaves + leaf, col, cols[r8, :])
            for k in range(2):
                for c in range(3):
                    src_rows[leaf, 2 * pair + k : 2 * pair + k + 1, c * size : (c + 1) * size] = (
                        jnp.sum(sums_src[k][c], axis=0, keepdims=True)
                    )

    near_t = jnp.transpose(cols[...])
    hot = jnp.transpose(hot_src[...].reshape(leaves * slots, 128)).astype(BF16)
    values = src_rows[...].reshape(leaves * slots, 3 * size)
    scattered = None
    for piece in pieces(values):
        term = dot(hot, piece.astype(BF16))
        scattered = term if scattered is None else scattered + term
    part_b[...] = scattered[:leaves]
    part_a[...] = scattered[2 * leaves : 3 * leaves]
    own = scattered[leaves : 2 * leaves]
    near = [
        near_t[c * leaves : (c + 1) * leaves] - own[:, c * size : (c + 1) * size]
        for c in range(3)
    ]
    for c in range(3):
        field[9 + c] = near[c]

    def part(k, src, dst, peer):
        return pltpu.make_async_remote_copy(
            src_ref=src,
            dst_ref=dst,
            send_sem=part_send.at[k],
            recv_sem=part_recv.at[k],
            device_id=(peer,),
            device_id_type=MESH,
        )

    part_left = part(0, part_b, got_a, me - 1)
    part_right = part(1, part_a, got_b, me + 1)

    @pl.when(has_left)
    def _():
        part_left.start()

    @pl.when(has_right)
    def _():
        part_right.start()

    gather(phases - 1).wait_recv()
    period = tiled.shape[1]
    spread_gap = iota((width, period), 1) - iota((width, period), 0)
    spread = spread_gap == 0
    for k in range(1, period // width):
        spread = spread | (spread_gap == k * width)
    spread = spread.astype(F32).astype(BF16)
    moments = mom[...].reshape(n * leaves, width)
    device = iota((1, n), 1)
    place_of = jnp.zeros((1, n), jnp.int32)
    for t in range(phases):
        bit = n >> (t + 1)
        mine = lax.rem(lax.div(me, bit), 2)
        theirs = lax.rem(lax.div(device, bit), 2)
        place_of = place_of + (theirs + mine - 2 * theirs * mine) * (1 << t)
    row_iota = iota((n * leaves, n), 0)
    picked = []
    for place in range(cap):
        wanted = place_of * leaves + req[place : place + 1, :]
        pick = (row_iota == wanted).astype(F32).astype(BF16)
        chosen = lax.dot_general(
            pick, moments, (((0,), (0,)), ((), ())), preferred_element_type=F32
        ).astype(BF16)
        picked.append(dot(chosen, spread).astype(BF16))
    chosen_rows = jnp.concatenate(picked, axis=0)
    for k in range(period // 128):
        lanes = slice(k * 128, (k + 1) * 128)
        tiled[:, lanes] = dot(hot_slot[...], chosen_rows[:, lanes])

    expan[...] = jnp.zeros_like(expan)
    step = 256 if block % 256 == 0 else 128
    per_block = block // width

    @pl.loop(0, width * width // block)
    def _(b):
        table_copy(b).wait()
        for t in range(block // step):
            start = pl.multiple_of(b * block + t * step, 128)
            oper = dot(hot_class[...], table[:, pl.ds(start, step)])
            for h in range(step // 128):
                tile = ((t * step) // 128 + h) % (period // 128)
                acc = None
                for s in range(far_num):
                    rows = slice(s * leaves, (s + 1) * leaves)
                    term = oper[rows, h * 128 : (h + 1) * 128] * tiled[
                        rows, tile * 128 : (tile + 1) * 128
                    ]
                    acc = term if acc is None else acc + term
                sums[:, t * step + h * 128 : t * step + (h + 1) * 128] = acc
        whole = sums[...]
        high = whole.astype(BF16)
        low = (whole - high.astype(F32)).astype(BF16)
        res = dot(high, fold[...]) + dot(low, fold[...])
        wide = jnp.concatenate([res, jnp.zeros((leaves, expan.shape[1] - 128), F32)], axis=1)
        expan[...] += pltpu.roll(wide, b * per_block, 1)

    expansion = expan[...][:, :width].astype(BF16)
    get_down.wait()
    leaf_row = iota((leaves, size), 0)
    for q in range(9):
        field[q] = jnp.zeros((leaves, size), F32)

    @pl.loop(0, leaves)
    def _(leaf):
        for q in range(9):
            got = dot(expansion, down[leaf, q])
            field[q] += jnp.where(leaf_row == leaf, got, 0.0)

    @pl.when(has_right)
    def _():
        part_left.wait_recv()

    @pl.when(jnp.logical_not(has_right))
    def _():
        got_a[...] = jnp.zeros_like(got_a)

    @pl.when(has_left)
    def _():
        part_right.wait_recv()

    @pl.when(jnp.logical_not(has_left))
    def _():
        got_b[...] = jnp.zeros_like(got_b)

    for k in range(3):
        lanes = slice(k * size, (k + 1) * size)
        result = field[9 + k] - (got_b[:, lanes] + got_a[:, lanes])
        for c in range(3):
            result = result + dens_rows[:, c * size : (c + 1) * size] * field[3 * c + k]
        for leaf in range(leaves):
            out[k : k + 1, leaf * size : (leaf + 1) * size] = result[leaf : leaf + 1]

    @pl.when(has_right)
    def _():
        part_right.wait_send()
        for copy in to_right:
            copy.wait_send()

    @pl.when(has_left)
    def _():
        part_left.wait_send()
        for copy in to_left:
            copy.wait_send()

    for t in range(phases):
        gather(t).wait_send()


def per_device(
    n,
    positions,
    densities,
    near_src,
    near_count,
    far_slot,
    far_class,
    far_count,
    requests,
    up_basis,
    transfer_table,
    down_basis,
):
    leaves, slots = near_src.shape
    nodes = positions.shape[1]
    size = nodes // leaves
    width = up_basis.shape[1]
    far_num = far_slot.shape[1]
    cap = requests.shape[2]
    classes = transfer_table.shape[0]
    phases = n.bit_length() - 1
    period = math.lcm(width, 128)
    blocks = width * width // period
    block = 2 * period if blocks % 2 == 0 else period
    down = jnp.transpose(down_basis, (0, 2, 1, 3))
    blocks = width * width // block
    smem = pl.BlockSpec(memory_space=pltpu.SMEM)
    vmem = pl.BlockSpec(memory_space=pltpu.VMEM)
    hbm = pl.BlockSpec(memory_space=pl.ANY)
    line = pltpu.VMEM((3, nodes), F32)
    part = pltpu.VMEM((leaves, 3 * size), F32)
    return pl.pallas_call(
        functools.partial(body, n),
        out_shape=jax.ShapeDtypeStruct((3, nodes), F32),
        in_specs=[smem] * 3 + [vmem] * 7 + [hbm] * 3,
        out_specs=vmem,
        scratch_shapes=[line] * 4
        + [
            pltpu.VMEM(up_basis.shape, BF16),
            pltpu.VMEM(transfer_table.shape, BF16),
            pltpu.VMEM(down.shape, BF16),
            part,
            pltpu.VMEM((n, leaves, width), BF16),
            pltpu.VMEM((ROWS, nodes), F32),
            pltpu.VMEM((ROWS, nodes), F32),
            pltpu.VMEM((3 * leaves + 1, 8, size), F32),
            pltpu.VMEM((3 * leaves + 1, FEATURES, 4 * size), BF16),
            pltpu.VMEM((leaves, size, 128), BF16),
            pltpu.VMEM((leaves, size, 6 * size), F32),
            pltpu.VMEM((2, size, 4 * size), F32),
            pltpu.VMEM((2, size, 4 * size), F32),
            pltpu.VMEM((3, size, size), F32),
            pltpu.VMEM((size, 128), F32),
            pltpu.VMEM((leaves, slots, 3 * size), F32),
            pltpu.VMEM((leaves, slots, 128), F32),
            part,
            part,
            part,
            part,
            pltpu.VMEM((far_num * leaves, classes), BF16),
            pltpu.VMEM((far_num * leaves, cap * n), BF16),
            pltpu.VMEM((far_num * leaves, period), F32),
            pltpu.VMEM((leaves, block), F32),
            pltpu.VMEM((block, 128), BF16),
            pltpu.VMEM((leaves, (width + 127) // 128 * 128), F32),
            pltpu.VMEM((12, leaves, size), F32),
            pltpu.SemaphoreType.DMA,
            pltpu.SemaphoreType.DMA((blocks,)),
            pltpu.SemaphoreType.DMA,
            pltpu.SemaphoreType.DMA((4,)),
            pltpu.SemaphoreType.DMA((4,)),
            pltpu.SemaphoreType.DMA((phases,)),
            pltpu.SemaphoreType.DMA((phases,)),
            pltpu.SemaphoreType.DMA((2,)),
            pltpu.SemaphoreType.DMA((2,)),
        ],
        compiler_params=pltpu.CompilerParams(
            collective_id=0, has_side_effects=True, vmem_limit_bytes=60 * 1024 * 1024
        ),
    )(
        near_src.T,
        near_count,
        far_count,
        positions,
        densities,
        far_slot,
        far_class,
        requests[0].T,
        jnp.asarray(source_choice(), BF16),
        jnp.asarray(target_choice(size), BF16),
        up_basis,
        transfer_table,
        down,
    )


def solution(mesh):
    placed = (
        P(None, "patch"),
        P(None, "patch"),
        P("patch", None),
        P("patch"),
        P("patch", None),
        P("patch", None),
        P("patch"),
        P("patch", None, None),
        P("patch", None, None),
        P(),
        P("patch", None, None, None),
    )
    return jax.shard_map(
        functools.partial(per_device, mesh.shape["patch"]),
        mesh=mesh,
        in_specs=placed,
        out_specs=P(None, "patch"),
        check_vma=False,
    )
```

```python
import functools
import math

import jax
import jax.numpy as jnp
import numpy as np
from jax import lax
from jax.experimental import pallas as pl
from jax.experimental.pallas import tpu as pltpu
from jax.sharding import PartitionSpec as P

KERNEL = 1.0 / (8.0 * math.pi)
BLOB = 0.25
MESH = pl.DeviceIdType.MESH
F32 = jnp.float32
BF16 = jnp.bfloat16

ROWS = 48
FEATURES = 48
LEFT = (0, 0, 0, 1, 1, 2)
RIGHT = (0, 1, 2, 0, 1, 0)


def at(group):
    return (group // 2) * 8 + (group % 2) * 3


def source_choice():
    sel = np.zeros((4, FEATURES, ROWS), np.float32)
    for k in range(6):
        for c in range(3):
            sel[0, 3 * k + c, at(3 + RIGHT[k]) + c] = 1.0
            sel[1, 3 * k + c, at(6 + RIGHT[k]) + c] = -1.0
            sel[2, 18 + 3 * k + c, at(RIGHT[k]) + c] = 1.0
            sel[3, 18 + 3 * k + c, at(6 + RIGHT[k]) + c] = -2.0
    for c in range(3):
        sel[1, 36 + c, at(11) + c] = 1.0
        sel[2, 42 + c, at(9) + c] = -1.0
        sel[3, 39 + c, at(11) + c] = 1.0
        sel[3, 42 + c, at(10) + c] = 1.0
    return sel.reshape(4 * FEATURES, ROWS)


def target_choice(size):
    sel = np.zeros((ROWS, 128), np.float32)
    spread = np.zeros((ROWS, 6, size), np.float32)
    for k in range(6):
        for c in range(3):
            sel[at(LEFT[k]) + c, 3 * k + c] = 1.0
            sel[at(3 + LEFT[k]) + c, 18 + 3 * k + c] = 1.0
    for c in range(3):
        sel[at(6) + c, 36 + c] = 1.0
        sel[at(7) + c, 39 + c] = 1.0
        sel[at(8) + c, 42 + c] = 1.0
        for piece in range(3):
            spread[at(3 + piece) + c, c, :] = 3.0
            spread[at(piece) + c, 3 + c, :] = 1.0
    return np.concatenate([sel, spread.reshape(ROWS, 6 * size)], axis=1)


def iota(shape, dim):
    return lax.broadcasted_iota(jnp.int32, shape, dim)


def dot(a, b):
    return jnp.dot(a, b, preferred_element_type=F32)


def pieces(x):
    high = x.astype(BF16).astype(F32)
    rest = x - high
    mid = rest.astype(BF16).astype(F32)
    return high, mid, rest - mid


def inner(a, b):
    return a[0:1] * b[0:1] + a[1:2] * b[1:2] + a[2:3] * b[2:3]


def put(rows, group, value):
    rows[at(group) : at(group) + value.shape[0], : value.shape[1]] = value


def put_pieces(rows, group, value):
    for k, piece in enumerate(pieces(value)):
        if value.shape[0] == 3:
            put(rows, group + k, piece)
        else:
            rows[at(group) + k : at(group) + k + 1, : value.shape[1]] = piece


def source_rows(rows, x, f):
    put_pieces(rows, 0, f)
    put_pieces(rows, 3, f * (1.0 / 3.0))
    put_pieces(rows, 6, x)
    put_pieces(rows, 9, inner(f, x))
    put_pieces(rows, 10, inner(x, x) + BLOB)
    put(rows, 11, jnp.ones_like(x))


def target_rows(rows, x, f):
    a = f * KERNEL
    put_pieces(rows, 0, a)
    put_pieces(rows, 3, x)
    put_pieces(rows, 6, inner(a, x))
    put_pieces(rows, 7, inner(x, x))
    put(rows, 8, jnp.ones_like(x))


def flip(me, bit):
    return me + bit - 2 * bit * lax.rem(lax.div(me, bit), 2)


def body(
    n,
    near_src,
    near_count,
    far_count,
    pos,
    dens,
    far_slot,
    far_class,
    req,
    choose_src,
    choose_tgt,
    up_hbm,
    table_hbm,
    down_hbm,
    out,
    pos_b,
    pos_a,
    dens_b,
    dens_a,
    up,
    table,
    down,
    dens_rows,
    mom,
    rows_own,
    rows_oth,
    window,
    rhs,
    lhs,
    tb,
    geo0,
    geo1,
    tacc,
    cols,
    src_rows,
    hot_src,
    part_b,
    part_a,
    got_b,
    got_a,
    hot_class,
    hot_slot,
    tiled,
    sums,
    fold,
    scatter,
    pick,
    spread,
    field,
    up_sem,
    table_sem,
    down_sem,
    halo_send,
    halo_recv,
    mom_send,
    mom_recv,
    part_send,
    part_recv,
):
    leaves, width = mom.shape[1:]
    nodes = pos.shape[1]
    size = nodes // leaves
    slots = near_src.shape[0]
    far_num = far_slot.shape[1]
    classes = table.shape[0]
    cap = req.shape[0]
    block = fold.shape[0]
    phases = n.bit_length() - 1
    expan_width = (width + 127) // 128 * 128
    me = lax.axis_index("patch")
    has_left = me > 0
    has_right = me < n - 1
    barrier = pltpu.get_barrier_semaphore()

    def signal(peer):
        pl.semaphore_signal(barrier, inc=1, device_id=(peer,), device_id_type=MESH)

    for t in range(phases):
        signal(flip(me, n >> (t + 1)))

    @pl.when(has_left)
    def _():
        signal(me - 1)

    @pl.when(has_right)
    def _():
        signal(me + 1)

    get_up = pltpu.make_async_copy(up_hbm, up, up_sem)
    get_up.start()

    def table_copy(b):
        lanes = pl.ds(pl.multiple_of(b * block, 128), block)
        return pltpu.make_async_copy(
            table_hbm.at[:, lanes], table.at[:, lanes], table_sem.at[b]
        )

    for b in range(width * width // block):
        table_copy(b).start()
    get_down = pltpu.make_async_copy(down_hbm, down, down_sem)
    get_down.start()

    for leaf in range(leaves):
        for c in range(3):
            dens_rows[leaf : leaf + 1, c * size : (c + 1) * size] = dens[
                c : c + 1, leaf * size : (leaf + 1) * size
            ]
    dens_round = dens_rows[...].astype(BF16)
    get_up.wait()
    row = iota((leaves, width), 0)
    total = jnp.zeros((leaves, width), F32)
    for leaf in range(leaves):
        got = lax.dot_general(
            dens_round, up[leaf], (((1,), (1,)), ((), ())), preferred_element_type=F32
        )
        total = total + jnp.where(row == leaf, got, 0.0)
    mom[0] = total.astype(BF16)

    def halo(k, src, dst, peer):
        return pltpu.make_async_remote_copy(
            src_ref=src,
            dst_ref=dst,
            send_sem=halo_send.at[k],
            recv_sem=halo_recv.at[k],
            device_id=(peer,),
            device_id_type=MESH,
        )

    to_right = (halo(0, pos, pos_b, me + 1), halo(1, dens, dens_b, me + 1))
    to_left = (halo(2, pos, pos_a, me - 1), halo(3, dens, dens_a, me - 1))

    def gather(t):
        return pltpu.make_async_remote_copy(
            src_ref=mom.at[0 : 1 << t],
            dst_ref=mom.at[1 << t : 2 << t],
            send_sem=mom_send.at[t],
            recv_sem=mom_recv.at[t],
            device_id=(flip(me, n >> (t + 1)),),
            device_id_type=MESH,
        )

    pl.semaphore_wait(
        barrier, phases + has_left.astype(jnp.int32) + has_right.astype(jnp.int32)
    )

    @pl.when(has_right)
    def _():
        for copy in to_right:
            copy.start()

    @pl.when(has_left)
    def _():
        for copy in to_left:
            copy.start()

    gather(0).start()

    rows_own[...] = jnp.zeros_like(rows_own)
    rows_oth[...] = jnp.zeros_like(rows_oth)
    target_rows(rows_own, pos[...], dens[...])

    few = 4

    @pl.loop(0, leaves // few)
    def _(group):
        turned = []
        for k in range(few):
            start = pl.multiple_of((group * few + k) * size, size)
            turned.append(jnp.transpose(rows_own[:, pl.ds(start, size)]).astype(BF16))
        turned = jnp.concatenate(turned, axis=0)
        spread_out = dot(turned, choose_tgt[...])
        for k in range(few):
            mine = spread_out[k * size : (k + 1) * size]
            lhs[group * few + k] = mine[:, :128].astype(BF16)
            tb[group * few + k] = mine[:, 128:]

    def sources(part, rows, x, f):
        source_rows(rows, x[...], f[...])
        for leaf in range(leaves):
            lanes = slice(leaf * size, (leaf + 1) * size)
            window[part * leaves + leaf, 0:3, :] = x[:, lanes] * 3.0
            window[part * leaves + leaf, 3:6, :] = f[:, lanes]

        for leaf in range(0, leaves, 2):
            chosen = dot(
                choose_src[...], rows[:, leaf * size : (leaf + 2) * size].astype(BF16)
            ).astype(BF16)
            for k in range(2):
                for o in range(4):
                    rhs[part * leaves + leaf + k, :, o * size : (o + 1) * size] = chosen[
                        o * FEATURES : (o + 1) * FEATURES, k * size : (k + 1) * size
                    ]

    window[...] = jnp.zeros_like(window)
    nothing = jnp.zeros((3, size), F32)
    source_rows(rows_oth, nothing, nothing)
    chosen = dot(choose_src[...], rows_oth[:, :size].astype(BF16)).astype(BF16)
    for o in range(4):
        rhs[3 * leaves, :, o * size : (o + 1) * size] = chosen[
            o * FEATURES : (o + 1) * FEATURES
        ]
    sources(1, rows_oth, pos, dens)

    count_col = jnp.zeros((leaves, 1), jnp.int32)
    leaf_col = iota((leaves, 1), 0)
    for leaf in range(leaves):
        count_col = jnp.where(leaf_col == leaf, far_count[leaf], count_col)
    class_iota = iota((leaves, classes), 1)
    column = iota((leaves, cap * n), 1)
    slot_of = lax.rem(column, n) * cap + lax.div(column, n)
    for s in range(far_num):
        rows = slice(s * leaves, (s + 1) * leaves)
        wanted = jnp.where(s < count_col, far_class[:, s : s + 1], -1)
        hot_class[rows, :] = (class_iota == wanted).astype(F32).astype(BF16)
        slot = far_slot[:, s : s + 1]
        hot_slot[rows, :] = (slot_of == slot).astype(F32).astype(BF16)
    fold_row = iota(fold.shape, 0)
    fold_first = iota(fold.shape, 1) * width
    fold[...] = (
        ((fold_row >= fold_first) & (fold_row < fold_first + width)).astype(F32).astype(BF16)
    )
    cols[...] = jnp.zeros_like(cols)
    offset = (me - 1) * leaves
    lane8 = iota((8, size), 1)
    lane1 = iota((1, 128), 1)

    def source_of(leaf, slot):
        live = slot < near_count[leaf]
        return jnp.where(live, near_src[slot, leaf] - offset, 3 * leaves)

    for leaf in range(leaves):
        for slot in range(slots):
            hot_src[leaf, slot : slot + 1, :] = (lane1 == source_of(leaf, slot)).astype(F32)
    scatter[...] = jnp.transpose(hot_src[...].reshape(leaves * slots, 128)).astype(BF16)

    device = iota((1, n), 1)
    place_of = jnp.zeros((1, n), jnp.int32)
    for t in range(phases):
        bit = n >> (t + 1)
        mine = lax.rem(lax.div(me, bit), 2)
        theirs = lax.rem(lax.div(device, bit), 2)
        place_of = place_of + (theirs + mine - 2 * theirs * mine) * (1 << t)
    row_iota = iota((n * leaves, n), 0)
    wanted = jnp.concatenate(
        [
            (row_iota == place_of * leaves + req[place : place + 1, :]).astype(F32)
            for place in range(cap)
        ],
        axis=1,
    )
    pick[...] = jnp.transpose(wanted).astype(BF16)
    period = tiled.shape[1]
    spread_gap = iota((width, period), 1) - iota((width, period), 0)
    near_gap = spread_gap == 0
    for k in range(1, period // width):
        near_gap = near_gap | (spread_gap == k * width)
    spread[...] = near_gap.astype(F32).astype(BF16)

    @pl.when(has_left)
    def _():
        for copy in to_right:
            copy.wait_recv()

    @pl.when(jnp.logical_not(has_left))
    def _():
        pos_b[...] = jnp.zeros_like(pos_b)
        dens_b[...] = jnp.zeros_like(dens_b)

    sources(0, rows_oth, pos_b, dens_b)

    @pl.when(has_right)
    def _():
        for copy in to_left:
            copy.wait_recv()

    @pl.when(jnp.logical_not(has_right))
    def _():
        pos_a[...] = jnp.zeros_like(pos_a)
        dens_a[...] = jnp.zeros_like(dens_a)

    sources(2, rows_own, pos_a, dens_a)

    def geometry(geo, leaf, first):
        for k in range(2):
            geo[k] = dot(lhs[leaf][:, :FEATURES], rhs[source_of(leaf, first + k)])

    geometry(geo0, 0, 0)
    pairs = slots // 2
    together = 2

    @pl.loop(0, leaves // together)
    def _(turn):
        for t in range(1, phases):
            @pl.when(turn == ((t - 1) * (leaves // together)) // max(phases - 1, 1))
            def _():
                gather(t - 1).wait_recv()
                gather(t).start()

        for sub in range(together * pairs):
            leaf = turn * together + sub // pairs
            pair = sub % pairs
            following = lax.rem(leaf + 1, leaves)
            geo, other = ((geo0, geo1), (geo1, geo0))[pair % 2]
            if pair + 1 < pairs:
                geometry(other, leaf, 2 * pair + 2)
            else:
                geometry(other, following, 0)
            xs, fs, sums_src = [], [], []
            for k in range(2):
                index = source_of(leaf, 2 * pair + k)
                nodes_k = window[index]
                xs.append([jnp.broadcast_to(nodes_k[c : c + 1], (8, size)) for c in range(3)])
                fs.append([jnp.broadcast_to(nodes_k[3 + c : 4 + c], (8, size)) for c in range(3)])
                sums_src.append([None] * 3)
            for g in range(size // 8):
                r8 = slice(g * 8, (g + 1) * 8)
                total = [None] * 3
                for k in range(2):
                    ab, ar, br, rho = [
                        geo[k, r8, o * size : (o + 1) * size] for o in range(4)
                    ]
                    inv1 = lax.rsqrt(rho)
                    inv2 = inv1 * inv1
                    inv3 = inv1 * inv2
                    p = br * inv3
                    q = ar * inv3
                    w = ab * inv3 + (p * ar) * inv2
                    for c in range(3):
                        sep = tb[leaf, r8, c * size : (c + 1) * size] - xs[k][c]
                        a = tb[leaf, r8, (3 + c) * size : (4 + c) * size]
                        term = a * p + fs[k][c] * q - w * sep
                        sums_src[k][c] = term if g == 0 else sums_src[k][c] + term
                        total[c] = term if k == 0 else total[c] + term
                for c in range(3):
                    if pair > 0:
                        total[c] = total[c] + tacc[c, r8, :]
                    if pair + 1 < pairs:
                        tacc[c, r8, :] = total[c]
                    else:
                        col = jnp.sum(total[c], axis=1, keepdims=True)
                        cols[r8, :] = jnp.where(lane8 == c * leaves + leaf, col, cols[r8, :])
            for k in range(2):
                for c in range(3):
                    src_rows[leaf, 2 * pair + k : 2 * pair + k + 1, c * size : (c + 1) * size] = (
                        jnp.sum(sums_src[k][c], axis=0, keepdims=True)
                    )

    near_t = jnp.transpose(cols[...])
    values = src_rows[...].reshape(leaves * slots, 3 * size)
    scattered = None
    for piece in pieces(values):
        term = dot(scatter[...], piece.astype(BF16))
        scattered = term if scattered is None else scattered + term
    part_b[...] = scattered[:leaves]
    part_a[...] = scattered[2 * leaves : 3 * leaves]
    own = scattered[leaves : 2 * leaves]
    near = [
        near_t[c * leaves : (c + 1) * leaves] - own[:, c * size : (c + 1) * size]
        for c in range(3)
    ]
    for c in range(3):
        field[9 + c] = near[c]

    def part(k, src, dst, peer):
        return pltpu.make_async_remote_copy(
            src_ref=src,
            dst_ref=dst,
            send_sem=part_send.at[k],
            recv_sem=part_recv.at[k],
            device_id=(peer,),
            device_id_type=MESH,
        )

    part_left = part(0, part_b, got_a, me - 1)
    part_right = part(1, part_a, got_b, me + 1)

    @pl.when(has_left)
    def _():
        part_left.start()

    @pl.when(has_right)
    def _():
        part_right.start()

    gather(phases - 1).wait_recv()
    moments = mom[...].reshape(n * leaves, width)
    chosen = dot(pick[...], moments).astype(BF16)
    chosen_rows = dot(chosen, spread[...]).astype(BF16)
    tiled[...] = dot(hot_slot[...], chosen_rows)

    step = 256 if block % 256 == 0 else 128
    per_block = block // width
    blocks = width * width // block
    joint = 3 if blocks % 3 == 0 else 1

    @pl.loop(0, blocks // joint)
    def _(turn):
        for k in range(joint):
            table_copy(turn * joint + k).wait()
        for k in range(joint):
            b = turn * joint + k
            lines = pl.ds(pl.multiple_of(b * leaves, leaves), leaves)
            for t in range(block // step):
                start = pl.multiple_of(b * block + t * step, 128)
                oper = dot(hot_class[...], table[:, pl.ds(start, step)])
                for h in range(step // 128):
                    tile = ((t * step) // 128 + h) % (period // 128)
                    acc = None
                    for s in range(far_num):
                        rows = slice(s * leaves, (s + 1) * leaves)
                        term = oper[rows, h * 128 : (h + 1) * 128] * tiled[
                            rows, tile * 128 : (tile + 1) * 128
                        ]
                        acc = term if acc is None else acc + term
                    sums[lines, t * step + h * 128 : t * step + (h + 1) * 128] = acc

    whole = sums[...]
    high = whole.astype(BF16)
    low = (whole - high.astype(F32)).astype(BF16)
    res = dot(high, fold[...]) + dot(low, fold[...])
    wide = jnp.zeros((leaves, expan_width), F32)
    for b in range(blocks):
        one = jnp.concatenate(
            [res[b * leaves : (b + 1) * leaves], jnp.zeros((leaves, expan_width - 128), F32)], axis=1
        )
        wide = wide + (pltpu.roll(one, b * per_block, 1) if b else one)
    expansion = wide[:, :width]
    get_down.wait()
    leaf_row = iota((leaves, width), 0)
    nothing = jnp.zeros_like(expansion)
    single = [
        jnp.where(leaf_row == leaf, expansion, nothing).astype(BF16) for leaf in range(leaves)
    ]
    for q in range(9):
        total = None
        for leaf in range(leaves):
            got = dot(single[leaf], down[leaf, q])
            total = got if total is None else total + got
        field[q] = total

    @pl.when(has_right)
    def _():
        part_left.wait_recv()

    @pl.when(jnp.logical_not(has_right))
    def _():
        got_a[...] = jnp.zeros_like(got_a)

    @pl.when(has_left)
    def _():
        part_right.wait_recv()

    @pl.when(jnp.logical_not(has_left))
    def _():
        got_b[...] = jnp.zeros_like(got_b)

    for k in range(3):
        lanes = slice(k * size, (k + 1) * size)
        result = field[9 + k] - (got_b[:, lanes] + got_a[:, lanes])
        for c in range(3):
            result = result + dens_rows[:, c * size : (c + 1) * size] * field[3 * c + k]
        for leaf in range(leaves):
            out[k : k + 1, leaf * size : (leaf + 1) * size] = result[leaf : leaf + 1]

    @pl.when(has_right)
    def _():
        part_right.wait_send()
        for copy in to_right:
            copy.wait_send()

    @pl.when(has_left)
    def _():
        part_left.wait_send()
        for copy in to_left:
            copy.wait_send()

    for t in range(phases):
        gather(t).wait_send()


def per_device(
    n,
    positions,
    densities,
    near_src,
    near_count,
    far_slot,
    far_class,
    far_count,
    requests,
    up_basis,
    transfer_table,
    down_basis,
):
    leaves, slots = near_src.shape
    nodes = positions.shape[1]
    size = nodes // leaves
    width = up_basis.shape[1]
    far_num = far_slot.shape[1]
    cap = requests.shape[2]
    classes = transfer_table.shape[0]
    phases = n.bit_length() - 1
    period = math.lcm(width, 128)
    blocks = width * width // period
    block = 2 * period if blocks % 2 == 0 else period
    down = jnp.transpose(down_basis, (0, 2, 1, 3))
    blocks = width * width // block
    smem = pl.BlockSpec(memory_space=pltpu.SMEM)
    vmem = pl.BlockSpec(memory_space=pltpu.VMEM)
    hbm = pl.BlockSpec(memory_space=pl.ANY)
    line = pltpu.VMEM((3, nodes), F32)
    part = pltpu.VMEM((leaves, 3 * size), F32)
    return pl.pallas_call(
        functools.partial(body, n),
        out_shape=jax.ShapeDtypeStruct((3, nodes), F32),
        in_specs=[smem] * 3 + [vmem] * 7 + [hbm] * 3,
        out_specs=vmem,
        scratch_shapes=[line] * 4
        + [
            pltpu.VMEM(up_basis.shape, BF16),
            pltpu.VMEM(transfer_table.shape, BF16),
            pltpu.VMEM(down.shape, BF16),
            part,
            pltpu.VMEM((n, leaves, width), BF16),
            pltpu.VMEM((ROWS, nodes), F32),
            pltpu.VMEM((ROWS, nodes), F32),
            pltpu.VMEM((3 * leaves + 1, 8, size), F32),
            pltpu.VMEM((3 * leaves + 1, FEATURES, 4 * size), BF16),
            pltpu.VMEM((leaves, size, 128), BF16),
            pltpu.VMEM((leaves, size, 6 * size), F32),
            pltpu.VMEM((2, size, 4 * size), F32),
            pltpu.VMEM((2, size, 4 * size), F32),
            pltpu.VMEM((3, size, size), F32),
            pltpu.VMEM((size, 128), F32),
            pltpu.VMEM((leaves, slots, 3 * size), F32),
            pltpu.VMEM((leaves, slots, 128), F32),
            part,
            part,
            part,
            part,
            pltpu.VMEM((far_num * leaves, classes), BF16),
            pltpu.VMEM((far_num * leaves, cap * n), BF16),
            pltpu.VMEM((far_num * leaves, period), F32),
            pltpu.VMEM((blocks * leaves, block), F32),
            pltpu.VMEM((block, 128), BF16),
            pltpu.VMEM((128, leaves * slots), BF16),
            pltpu.VMEM((cap * n, n * leaves), BF16),
            pltpu.VMEM((width, period), BF16),
            pltpu.VMEM((12, leaves, size), F32),
            pltpu.SemaphoreType.DMA,
            pltpu.SemaphoreType.DMA((blocks,)),
            pltpu.SemaphoreType.DMA,
            pltpu.SemaphoreType.DMA((4,)),
            pltpu.SemaphoreType.DMA((4,)),
            pltpu.SemaphoreType.DMA((phases,)),
            pltpu.SemaphoreType.DMA((phases,)),
            pltpu.SemaphoreType.DMA((2,)),
            pltpu.SemaphoreType.DMA((2,)),
        ],
        compiler_params=pltpu.CompilerParams(
            collective_id=0, has_side_effects=True, vmem_limit_bytes=60 * 1024 * 1024
        ),
    )(
        near_src.T,
        near_count,
        far_count,
        positions,
        densities,
        far_slot,
        far_class,
        requests[0].T,
        jnp.asarray(source_choice(), BF16),
        jnp.asarray(target_choice(size), BF16),
        up_basis,
        transfer_table,
        down,
    )


def solution(mesh):
    placed = (
        P(None, "patch"),
        P(None, "patch"),
        P("patch", None),
        P("patch"),
        P("patch", None),
        P("patch", None),
        P("patch"),
        P("patch", None, None),
        P("patch", None, None),
        P(),
        P("patch", None, None, None),
    )
    return jax.shard_map(
        functools.partial(per_device, mesh.shape["patch"]),
        mesh=mesh,
        in_specs=placed,
        out_specs=P(None, "patch"),
        check_vma=False,
    )
```

```python
import functools
import math

import jax
import jax.numpy as jnp
import numpy as np
from jax import lax
from jax.experimental import pallas as pl
from jax.experimental.pallas import tpu as pltpu
from jax.sharding import PartitionSpec as P

KERNEL = 1.0 / (8.0 * math.pi)
BLOB = 0.25
MESH = pl.DeviceIdType.MESH
F32 = jnp.float32
BF16 = jnp.bfloat16

ROWS = 48
FEATURES = 48
LEFT = (0, 0, 0, 1, 1, 2)
RIGHT = (0, 1, 2, 0, 1, 0)


def at(group):
    return (group // 2) * 8 + (group % 2) * 3


def source_choice():
    sel = np.zeros((4, FEATURES, ROWS), np.float32)
    for k in range(6):
        for c in range(3):
            sel[0, 3 * k + c, at(3 + RIGHT[k]) + c] = 1.0
            sel[1, 3 * k + c, at(6 + RIGHT[k]) + c] = -1.0
            sel[2, 18 + 3 * k + c, at(RIGHT[k]) + c] = 1.0
            sel[3, 18 + 3 * k + c, at(6 + RIGHT[k]) + c] = -2.0
    for c in range(3):
        sel[1, 36 + c, at(11) + c] = 1.0
        sel[2, 42 + c, at(9) + c] = -1.0
        sel[3, 39 + c, at(11) + c] = 1.0
        sel[3, 42 + c, at(10) + c] = 1.0
    return sel.reshape(4 * FEATURES, ROWS)


def target_choice(size):
    sel = np.zeros((ROWS, 128), np.float32)
    spread = np.zeros((ROWS, 6, size), np.float32)
    for k in range(6):
        for c in range(3):
            sel[at(LEFT[k]) + c, 3 * k + c] = 1.0
            sel[at(3 + LEFT[k]) + c, 18 + 3 * k + c] = 1.0
    for c in range(3):
        sel[at(6) + c, 36 + c] = 1.0
        sel[at(7) + c, 39 + c] = 1.0
        sel[at(8) + c, 42 + c] = 1.0
        for piece in range(3):
            spread[at(3 + piece) + c, c, :] = 3.0
            spread[at(piece) + c, 3 + c, :] = 1.0
    return np.concatenate([sel, spread.reshape(ROWS, 6 * size)], axis=1)


def iota(shape, dim):
    return lax.broadcasted_iota(jnp.int32, shape, dim)


def dot(a, b):
    return jnp.dot(a, b, preferred_element_type=F32)


def pieces(x):
    high = x.astype(BF16).astype(F32)
    rest = x - high
    mid = rest.astype(BF16).astype(F32)
    return high, mid, rest - mid


def inner(a, b):
    return a[0:1] * b[0:1] + a[1:2] * b[1:2] + a[2:3] * b[2:3]


def put(rows, group, value):
    rows[at(group) : at(group) + value.shape[0], : value.shape[1]] = value


def put_pieces(rows, group, value):
    for k, piece in enumerate(pieces(value)):
        if value.shape[0] == 3:
            put(rows, group + k, piece)
        else:
            rows[at(group) + k : at(group) + k + 1, : value.shape[1]] = piece


def source_rows(rows, x, f):
    put_pieces(rows, 0, f)
    put_pieces(rows, 3, f * (1.0 / 3.0))
    put_pieces(rows, 6, x)
    put_pieces(rows, 9, inner(f, x))
    put_pieces(rows, 10, inner(x, x) + BLOB)
    put(rows, 11, jnp.ones_like(x))


def target_rows(rows, x, f):
    a = f * KERNEL
    put_pieces(rows, 0, a)
    put_pieces(rows, 3, x)
    put_pieces(rows, 6, inner(a, x))
    put_pieces(rows, 7, inner(x, x))
    put(rows, 8, jnp.ones_like(x))


def flip(me, bit):
    return me + bit - 2 * bit * lax.rem(lax.div(me, bit), 2)


def body(
    n,
    near_src_hbm,
    near_count_hbm,
    far_count_hbm,
    pos_hbm,
    dens_hbm,
    far_slot_hbm,
    far_class_hbm,
    req_hbm,
    choose_src_hbm,
    choose_tgt_hbm,
    up_hbm,
    table_hbm,
    down_hbm,
    out,
    near_src,
    near_count,
    far_count,
    pos,
    dens,
    far_slot,
    far_class,
    req,
    choose_src,
    choose_tgt,
    pos_b,
    pos_a,
    dens_b,
    dens_a,
    up,
    table,
    down,
    dens_rows,
    mom,
    rows_own,
    rows_oth,
    window,
    rhs,
    lhs,
    tb,
    geo0,
    geo1,
    tacc,
    cols,
    src_rows,
    hot_src,
    part_b,
    part_a,
    got_b,
    got_a,
    hot_class,
    hot_slot,
    ready,
    tiled,
    sums,
    fold,
    scatter,
    pick,
    spread,
    field,
    in_sem,
    up_sem,
    table_sem,
    down_sem,
    halo_send,
    halo_recv,
    mom_send,
    mom_recv,
    part_send,
    part_recv,
):
    leaves, width = mom.shape[1:]
    nodes = pos.shape[1]
    size = nodes // leaves
    slots = near_src.shape[0]
    far_num = far_slot.shape[1]
    classes = table.shape[0]
    cap = req.shape[0]
    block = fold.shape[0]
    phases = n.bit_length() - 1
    expan_width = (width + 127) // 128 * 128
    me = lax.axis_index("patch")
    has_left = me > 0
    has_right = me < n - 1
    barrier = pltpu.get_barrier_semaphore()

    def signal(peer):
        pl.semaphore_signal(barrier, inc=1, device_id=(peer,), device_id_type=MESH)

    for t in range(phases):
        signal(flip(me, n >> (t + 1)))

    @pl.when(has_left)
    def _():
        signal(me - 1)

    @pl.when(has_right)
    def _():
        signal(me + 1)

    ins = [
        pltpu.make_async_copy(src, dst, in_sem.at[k])
        for k, (src, dst) in enumerate(
            (
                (pos_hbm, pos),
                (dens_hbm, dens),
                (choose_tgt_hbm, choose_tgt),
                (near_src_hbm, near_src),
                (near_count_hbm, near_count),
                (far_count_hbm, far_count),
                (far_slot_hbm, far_slot),
                (far_class_hbm, far_class),
                (req_hbm, req),
                (choose_src_hbm, choose_src),
            )
        )
    ]
    for copy in ins:
        copy.start()
    get_up = pltpu.make_async_copy(up_hbm, up, up_sem)
    get_up.start()

    def table_copy(b):
        lanes = pl.ds(pl.multiple_of(b * block, 128), block)
        return pltpu.make_async_copy(
            table_hbm.at[:, lanes], table.at[:, lanes], table_sem.at[b]
        )

    get_down = pltpu.make_async_copy(down_hbm, down, down_sem)
    for copy in ins:
        copy.wait()

    def halo(k, src, dst, peer):
        return pltpu.make_async_remote_copy(
            src_ref=src,
            dst_ref=dst,
            send_sem=halo_send.at[k],
            recv_sem=halo_recv.at[k],
            device_id=(peer,),
            device_id_type=MESH,
        )

    to_right = (halo(0, pos, pos_b, me + 1), halo(1, dens, dens_b, me + 1))
    to_left = (halo(2, pos, pos_a, me - 1), halo(3, dens, dens_a, me - 1))

    def gather(t):
        return pltpu.make_async_remote_copy(
            src_ref=mom.at[0 : 1 << t],
            dst_ref=mom.at[1 << t : 2 << t],
            send_sem=mom_send.at[t],
            recv_sem=mom_recv.at[t],
            device_id=(flip(me, n >> (t + 1)),),
            device_id_type=MESH,
        )

    for leaf in range(leaves):
        for c in range(3):
            dens_rows[leaf : leaf + 1, c * size : (c + 1) * size] = dens[
                c : c + 1, leaf * size : (leaf + 1) * size
            ]
    dens_round = dens_rows[...].astype(BF16)
    get_up.wait()
    for b in range(width * width // block):
        table_copy(b).start()
    get_down.start()
    row = iota((leaves, width), 0)
    total = jnp.zeros((leaves, width), F32)
    for leaf in range(leaves):
        got = lax.dot_general(
            dens_round, up[leaf], (((1,), (1,)), ((), ())), preferred_element_type=F32
        )
        total = total + jnp.where(row == leaf, got, 0.0)
    mom[0] = total.astype(BF16)

    pl.semaphore_wait(
        barrier, phases + has_left.astype(jnp.int32) + has_right.astype(jnp.int32)
    )

    @pl.when(has_right)
    def _():
        for copy in to_right:
            copy.start()

    @pl.when(has_left)
    def _():
        for copy in to_left:
            copy.start()


    gather(0).start()

    rows_own[...] = jnp.zeros_like(rows_own)
    rows_oth[...] = jnp.zeros_like(rows_oth)
    target_rows(rows_own, pos[...], dens[...])

    few = 4

    @pl.loop(0, leaves // few)
    def _(group):
        turned = []
        for k in range(few):
            start = pl.multiple_of((group * few + k) * size, size)
            turned.append(jnp.transpose(rows_own[:, pl.ds(start, size)]).astype(BF16))
        turned = jnp.concatenate(turned, axis=0)
        spread_out = dot(turned, choose_tgt[...])
        for k in range(few):
            mine = spread_out[k * size : (k + 1) * size]
            lhs[group * few + k] = mine[:, :128].astype(BF16)
            tb[group * few + k] = mine[:, 128:]

    def sources(part, rows, x, f):
        source_rows(rows, x[...], f[...])
        for leaf in range(leaves):
            lanes = slice(leaf * size, (leaf + 1) * size)
            window[part * leaves + leaf, 0:3, :] = x[:, lanes] * 3.0
            window[part * leaves + leaf, 3:6, :] = f[:, lanes]

        for leaf in range(0, leaves, 2):
            chosen = dot(
                choose_src[...], rows[:, leaf * size : (leaf + 2) * size].astype(BF16)
            ).astype(BF16)
            for k in range(2):
                for o in range(4):
                    rhs[part * leaves + leaf + k, :, o * size : (o + 1) * size] = chosen[
                        o * FEATURES : (o + 1) * FEATURES, k * size : (k + 1) * size
                    ]

    window[...] = jnp.zeros_like(window)
    nothing = jnp.zeros((3, size), F32)
    source_rows(rows_oth, nothing, nothing)
    chosen = dot(choose_src[...], rows_oth[:, :size].astype(BF16)).astype(BF16)
    for o in range(4):
        rhs[3 * leaves, :, o * size : (o + 1) * size] = chosen[
            o * FEATURES : (o + 1) * FEATURES
        ]
    sources(1, rows_oth, pos, dens)

    count_col = jnp.zeros((leaves, 1), jnp.int32)
    leaf_col = iota((leaves, 1), 0)
    for leaf in range(leaves):
        count_col = jnp.where(leaf_col == leaf, far_count[leaf], count_col)
    class_iota = iota((leaves, classes), 1)
    column = iota((leaves, cap * n), 1)
    slot_of = lax.rem(column, n) * cap + lax.div(column, n)
    for s in range(far_num):
        rows = slice(s * leaves, (s + 1) * leaves)
        wanted = jnp.where(s < count_col, far_class[:, s : s + 1], -1)
        hot_class[rows, :] = (class_iota == wanted).astype(F32).astype(BF16)
        slot = far_slot[:, s : s + 1]
        hot_slot[rows, :] = (slot_of == slot).astype(F32).astype(BF16)
    fold_row = iota(fold.shape, 0)
    fold_first = iota(fold.shape, 1) * width
    fold[...] = (
        ((fold_row >= fold_first) & (fold_row < fold_first + width)).astype(F32).astype(BF16)
    )
    cols[...] = jnp.zeros_like(cols)
    offset = (me - 1) * leaves
    lane8 = iota((8, size), 1)
    lane1 = iota((1, 128), 1)

    def source_of(leaf, slot):
        live = slot < near_count[leaf]
        return jnp.where(live, near_src[slot, leaf] - offset, 3 * leaves)

    for leaf in range(leaves):
        for slot in range(slots):
            hot_src[leaf, slot : slot + 1, :] = (lane1 == source_of(leaf, slot)).astype(F32)
    scatter[...] = jnp.transpose(hot_src[...].reshape(leaves * slots, 128)).astype(BF16)

    device = iota((1, n), 1)
    place_of = jnp.zeros((1, n), jnp.int32)
    for t in range(phases):
        bit = n >> (t + 1)
        mine = lax.rem(lax.div(me, bit), 2)
        theirs = lax.rem(lax.div(device, bit), 2)
        place_of = place_of + (theirs + mine - 2 * theirs * mine) * (1 << t)
    row_iota = iota((n * leaves, n), 0)
    wanted = jnp.concatenate(
        [
            (row_iota == place_of * leaves + req[place : place + 1, :]).astype(F32)
            for place in range(cap)
        ],
        axis=1,
    )
    pick[...] = jnp.transpose(wanted).astype(BF16)
    period = tiled.shape[1]
    spread_gap = iota((width, period), 1) - iota((width, period), 0)
    near_gap = spread_gap == 0
    for k in range(1, period // width):
        near_gap = near_gap | (spread_gap == k * width)
    spread[...] = near_gap.astype(F32).astype(BF16)

    @pl.when(has_left)
    def _():
        for copy in to_right:
            copy.wait_recv()

    @pl.when(jnp.logical_not(has_left))
    def _():
        pos_b[...] = jnp.zeros_like(pos_b)
        dens_b[...] = jnp.zeros_like(dens_b)

    sources(0, rows_oth, pos_b, dens_b)

    @pl.when(has_right)
    def _():
        for copy in to_left:
            copy.wait_recv()

    @pl.when(jnp.logical_not(has_right))
    def _():
        pos_a[...] = jnp.zeros_like(pos_a)
        dens_a[...] = jnp.zeros_like(dens_a)

    sources(2, rows_own, pos_a, dens_a)

    group = 1
    steps = slots // group
    together = 4

    def geometry(geo, leaf, first):
        for k in range(group):
            geo[k] = dot(lhs[leaf][:, :FEATURES], rhs[source_of(leaf, first + k)])

    step = 256 if block % 256 == 0 else 128
    per_block = block // width
    blocks = width * width // block
    geometry(geo0, 0, 0)

    @pl.loop(0, leaves // together)
    def _(turn):
        for t in range(1, phases):
            @pl.when(turn == ((t - 1) * (leaves // together)) // max(phases - 1, 1))
            def _():
                gather(t - 1).wait_recv()
                gather(t).start()

        table_copy(turn).wait()
        for sub in range(together * steps):
            leaf = turn * together + sub // steps
            step_now = sub % steps
            geo, other = ((geo0, geo1), (geo1, geo0))[sub % 2]
            if sub + 1 < together * steps:
                nxt = sub + 1
                geometry(other, turn * together + nxt // steps, group * (nxt % steps))
            else:
                geometry(other, lax.rem((turn + 1) * together, leaves), 0)
            if sub % 3 == 0 and sub // 3 < block // step:
                start = pl.multiple_of(turn * block + (sub // 3) * step, 128)
                ready[turn, :, (sub // 3) * step : (sub // 3 + 1) * step] = dot(
                    hot_class[...], table[:, pl.ds(start, step)]
                )
            xs, fs, sums_src = [], [], []
            for k in range(group):
                index = source_of(leaf, group * step_now + k)
                nodes_k = window[index]
                xs.append([jnp.broadcast_to(nodes_k[c : c + 1], (8, size)) for c in range(3)])
                fs.append([jnp.broadcast_to(nodes_k[3 + c : 4 + c], (8, size)) for c in range(3)])
                sums_src.append([None] * 3)
            for g in range(size // 8):
                r8 = slice(g * 8, (g + 1) * 8)
                total = [None] * 3
                for k in range(group):
                    ab, ar, br, rho = [
                        geo[k, r8, o * size : (o + 1) * size] for o in range(4)
                    ]
                    inv1 = lax.rsqrt(rho)
                    inv2 = inv1 * inv1
                    inv3 = inv1 * inv2
                    p = br * inv3
                    q = ar * inv3
                    w = ab * inv3 + (p * ar) * inv2
                    for c in range(3):
                        sep = tb[leaf, r8, c * size : (c + 1) * size] - xs[k][c]
                        a = tb[leaf, r8, (3 + c) * size : (4 + c) * size]
                        term = a * p + fs[k][c] * q - w * sep
                        sums_src[k][c] = term if g == 0 else sums_src[k][c] + term
                        total[c] = term if k == 0 else total[c] + term
                for c in range(3):
                    if step_now > 0:
                        total[c] = total[c] + tacc[c, r8, :]
                    if step_now + 1 < steps:
                        tacc[c, r8, :] = total[c]
                    else:
                        col = jnp.sum(total[c], axis=1, keepdims=True)
                        cols[r8, :] = jnp.where(lane8 == c * leaves + leaf, col, cols[r8, :])
            for k in range(group):
                at_k = group * step_now + k
                for c in range(3):
                    src_rows[leaf, at_k : at_k + 1, c * size : (c + 1) * size] = jnp.sum(
                        sums_src[k][c], axis=0, keepdims=True
                    )

    near_t = jnp.transpose(cols[...])
    values = src_rows[...].reshape(leaves * slots, 3 * size)
    scattered = None
    for piece in pieces(values):
        term = dot(scatter[...], piece.astype(BF16))
        scattered = term if scattered is None else scattered + term
    part_b[...] = scattered[:leaves]
    part_a[...] = scattered[2 * leaves : 3 * leaves]
    own = scattered[leaves : 2 * leaves]
    near = [
        near_t[c * leaves : (c + 1) * leaves] - own[:, c * size : (c + 1) * size]
        for c in range(3)
    ]
    for c in range(3):
        field[9 + c] = near[c]

    def part(k, src, dst, peer):
        return pltpu.make_async_remote_copy(
            src_ref=src,
            dst_ref=dst,
            send_sem=part_send.at[k],
            recv_sem=part_recv.at[k],
            device_id=(peer,),
            device_id_type=MESH,
        )

    part_left = part(0, part_b, got_a, me - 1)
    part_right = part(1, part_a, got_b, me + 1)

    @pl.when(has_left)
    def _():
        part_left.start()

    @pl.when(has_right)
    def _():
        part_right.start()

    gather(phases - 1).wait_recv()
    moments = mom[...].reshape(n * leaves, width)
    chosen = dot(pick[...], moments).astype(BF16)
    chosen_rows = dot(chosen, spread[...]).astype(BF16)
    tiled[...] = dot(hot_slot[...], chosen_rows)


    early = ready.shape[0]

    def apply(members, t):
        for h in range(step // 128):
            tile = ((t * step) // 128 + h) % (period // 128)
            acc = [None] * len(members)
            for s in range(far_num):
                rows = slice(s * leaves, (s + 1) * leaves)
                factor = tiled[rows, tile * 128 : (tile + 1) * 128]
                for k, (b, oper) in enumerate(members):
                    term = oper(rows, h) * factor
                    acc[k] = term if acc[k] is None else acc[k] + term
            for k, (b, oper) in enumerate(members):
                lines = pl.ds(pl.multiple_of(b * leaves, leaves), leaves)
                sums[lines, t * step + h * 128 : t * step + (h + 1) * 128] = acc[k]

    def fresh(b, t):
        start = pl.multiple_of(b * block + t * step, 128)
        oper = dot(hot_class[...], table[:, pl.ds(start, step)])
        return b, lambda rows, h: oper[rows, h * 128 : (h + 1) * 128]

    def stored(b, t):
        return b, lambda rows, h: ready[
            b, rows, t * step + h * 128 : t * step + (h + 1) * 128
        ]

    paired = min(early, blocks - early)

    @pl.loop(0, paired)
    def _(b):
        table_copy(early + b).wait()
        for t in range(block // step):
            apply((fresh(early + b, t), stored(b, t)), t)

    for b in range(early + paired, blocks):
        table_copy(b).wait()
        for t in range(block // step):
            apply((fresh(b, t),), t)

    whole = sums[...]
    high = whole.astype(BF16)
    low = (whole - high.astype(F32)).astype(BF16)
    res = dot(high, fold[...]) + dot(low, fold[...])
    wide = jnp.zeros((leaves, expan_width), F32)
    for b in range(blocks):
        one = jnp.concatenate(
            [res[b * leaves : (b + 1) * leaves], jnp.zeros((leaves, expan_width - 128), F32)], axis=1
        )
        wide = wide + (pltpu.roll(one, b * per_block, 1) if b else one)
    expansion = wide[:, :width]
    get_down.wait()
    leaf_row = iota((leaves, width), 0)
    nothing = jnp.zeros_like(expansion)
    single = [
        jnp.where(leaf_row == leaf, expansion, nothing).astype(BF16) for leaf in range(leaves)
    ]
    for q in range(9):
        total = None
        for leaf in range(leaves):
            got = dot(single[leaf], down[leaf, q])
            total = got if total is None else total + got
        field[q] = total

    @pl.when(has_right)
    def _():
        part_left.wait_recv()

    @pl.when(jnp.logical_not(has_right))
    def _():
        got_a[...] = jnp.zeros_like(got_a)

    @pl.when(has_left)
    def _():
        part_right.wait_recv()

    @pl.when(jnp.logical_not(has_left))
    def _():
        got_b[...] = jnp.zeros_like(got_b)

    for k in range(3):
        lanes = slice(k * size, (k + 1) * size)
        result = field[9 + k] - (got_b[:, lanes] + got_a[:, lanes])
        for c in range(3):
            result = result + dens_rows[:, c * size : (c + 1) * size] * field[3 * c + k]
        for leaf in range(leaves):
            out[k : k + 1, leaf * size : (leaf + 1) * size] = result[leaf : leaf + 1]

    @pl.when(has_right)
    def _():
        part_right.wait_send()
        for copy in to_right:
            copy.wait_send()

    @pl.when(has_left)
    def _():
        part_left.wait_send()
        for copy in to_left:
            copy.wait_send()

    for t in range(phases):
        gather(t).wait_send()


def per_device(
    n,
    positions,
    densities,
    near_src,
    near_count,
    far_slot,
    far_class,
    far_count,
    requests,
    up_basis,
    transfer_table,
    down_basis,
):
    leaves, slots = near_src.shape
    nodes = positions.shape[1]
    size = nodes // leaves
    width = up_basis.shape[1]
    far_num = far_slot.shape[1]
    cap = requests.shape[2]
    classes = transfer_table.shape[0]
    phases = n.bit_length() - 1
    period = math.lcm(width, 128)
    blocks = width * width // period
    block = 2 * period if blocks % 2 == 0 else period
    down = jnp.transpose(down_basis, (0, 2, 1, 3))
    blocks = width * width // block
    vmem = pl.BlockSpec(memory_space=pltpu.VMEM)
    hbm = pl.BlockSpec(memory_space=pl.ANY)
    line = pltpu.VMEM((3, nodes), F32)
    part = pltpu.VMEM((leaves, 3 * size), F32)
    return pl.pallas_call(
        functools.partial(body, n),
        out_shape=pltpu.VMEM((3, nodes), F32),
        in_specs=[hbm] * 13,
        out_specs=vmem,
        scratch_shapes=[
            pltpu.SMEM((slots, leaves), jnp.int32),
            pltpu.SMEM((leaves,), jnp.int32),
            pltpu.SMEM((leaves,), jnp.int32),
            line,
            line,
            pltpu.VMEM(far_slot.shape, jnp.int32),
            pltpu.VMEM(far_class.shape, jnp.int32),
            pltpu.VMEM((cap, n), jnp.int32),
            pltpu.VMEM((4 * FEATURES, ROWS), BF16),
            pltpu.VMEM((ROWS, 128 + 6 * size), BF16),
        ]
        + [line] * 4
        + [
            pltpu.VMEM(up_basis.shape, BF16),
            pltpu.VMEM(transfer_table.shape, BF16),
            pltpu.VMEM(down.shape, BF16),
            part,
            pltpu.VMEM((n, leaves, width), BF16),
            pltpu.VMEM((ROWS, nodes), F32),
            pltpu.VMEM((ROWS, nodes), F32),
            pltpu.VMEM((3 * leaves + 1, 8, size), F32),
            pltpu.VMEM((3 * leaves + 1, FEATURES, 4 * size), BF16),
            pltpu.VMEM((leaves, size, 128), BF16),
            pltpu.VMEM((leaves, size, 6 * size), F32),
            pltpu.VMEM((2, size, 4 * size), F32),
            pltpu.VMEM((2, size, 4 * size), F32),
            pltpu.VMEM((3, size, size), F32),
            pltpu.VMEM((size, 128), F32),
            pltpu.VMEM((leaves, slots, 3 * size), F32),
            pltpu.VMEM((leaves, slots, 128), F32),
            part,
            part,
            part,
            part,
            pltpu.VMEM((far_num * leaves, classes), BF16),
            pltpu.VMEM((far_num * leaves, cap * n), BF16),
            pltpu.VMEM((leaves // 4, far_num * leaves, block), F32),
            pltpu.VMEM((far_num * leaves, period), F32),
            pltpu.VMEM((blocks * leaves, block), F32),
            pltpu.VMEM((block, 128), BF16),
            pltpu.VMEM((128, leaves * slots), BF16),
            pltpu.VMEM((cap * n, n * leaves), BF16),
            pltpu.VMEM((width, period), BF16),
            pltpu.VMEM((12, leaves, size), F32),
            pltpu.SemaphoreType.DMA((10,)),
            pltpu.SemaphoreType.DMA,
            pltpu.SemaphoreType.DMA((blocks,)),
            pltpu.SemaphoreType.DMA,
            pltpu.SemaphoreType.DMA((4,)),
            pltpu.SemaphoreType.DMA((4,)),
            pltpu.SemaphoreType.DMA((phases,)),
            pltpu.SemaphoreType.DMA((phases,)),
            pltpu.SemaphoreType.DMA((2,)),
            pltpu.SemaphoreType.DMA((2,)),
        ],
        compiler_params=pltpu.CompilerParams(
            collective_id=0, has_side_effects=True, vmem_limit_bytes=60 * 1024 * 1024
        ),
    )(
        near_src.T,
        near_count,
        far_count,
        positions,
        densities,
        far_slot,
        far_class,
        requests[0].T,
        jnp.asarray(source_choice(), BF16),
        jnp.asarray(target_choice(size), BF16),
        up_basis,
        transfer_table,
        down,
    )


def solution(mesh):
    placed = (
        P(None, "patch"),
        P(None, "patch"),
        P("patch", None),
        P("patch"),
        P("patch", None),
        P("patch", None),
        P("patch"),
        P("patch", None, None),
        P("patch", None, None),
        P(),
        P("patch", None, None, None),
    )
    return jax.shard_map(
        functools.partial(per_device, mesh.shape["patch"]),
        mesh=mesh,
        in_specs=placed,
        out_specs=P(None, "patch"),
        check_vma=False,
    )
```

```python
import functools
import math

import jax
import jax.numpy as jnp
import numpy as np
from jax import lax
from jax.experimental import pallas as pl
from jax.experimental.pallas import tpu as pltpu
from jax.sharding import PartitionSpec as P

KERNEL = 1.0 / (8.0 * math.pi)
BLOB = 0.25
MESH = pl.DeviceIdType.MESH
F32 = jnp.float32
BF16 = jnp.bfloat16

ROWS = 48
FEATURES = 48
LEFT = (0, 0, 0, 1, 1, 2)
RIGHT = (0, 1, 2, 0, 1, 0)


def at(group):
    return (group // 2) * 8 + (group % 2) * 3


def source_choice():
    sel = np.zeros((4, FEATURES, ROWS), np.float32)
    for k in range(6):
        for c in range(3):
            sel[0, 3 * k + c, at(3 + RIGHT[k]) + c] = 1.0
            sel[1, 3 * k + c, at(6 + RIGHT[k]) + c] = -1.0
            sel[2, 18 + 3 * k + c, at(RIGHT[k]) + c] = 1.0
            sel[3, 18 + 3 * k + c, at(6 + RIGHT[k]) + c] = -2.0
    for c in range(3):
        sel[1, 36 + c, at(11) + c] = 1.0
        sel[2, 42 + c, at(9) + c] = -1.0
        sel[3, 39 + c, at(11) + c] = 1.0
        sel[3, 42 + c, at(10) + c] = 1.0
    return sel.reshape(4 * FEATURES, ROWS)


def target_choice(size):
    sel = np.zeros((ROWS, 128), np.float32)
    spread = np.zeros((ROWS, 6, size), np.float32)
    for k in range(6):
        for c in range(3):
            sel[at(LEFT[k]) + c, 3 * k + c] = 1.0
            sel[at(3 + LEFT[k]) + c, 18 + 3 * k + c] = 1.0
    for c in range(3):
        sel[at(6) + c, 36 + c] = 1.0
        sel[at(7) + c, 39 + c] = 1.0
        sel[at(8) + c, 42 + c] = 1.0
        for piece in range(3):
            spread[at(3 + piece) + c, c, :] = 3.0
            spread[at(piece) + c, 3 + c, :] = 1.0
    return np.concatenate([sel, spread.reshape(ROWS, 6 * size)], axis=1)


def iota(shape, dim):
    return lax.broadcasted_iota(jnp.int32, shape, dim)


def dot(a, b):
    return jnp.dot(a, b, preferred_element_type=F32)


def pieces(x):
    high = x.astype(BF16).astype(F32)
    rest = x - high
    mid = rest.astype(BF16).astype(F32)
    return high, mid, rest - mid


def inner(a, b):
    return a[0:1] * b[0:1] + a[1:2] * b[1:2] + a[2:3] * b[2:3]


def put(rows, group, value):
    rows[at(group) : at(group) + value.shape[0], : value.shape[1]] = value


def put_pieces(rows, group, value):
    for k, piece in enumerate(pieces(value)):
        if value.shape[0] == 3:
            put(rows, group + k, piece)
        else:
            rows[at(group) + k : at(group) + k + 1, : value.shape[1]] = piece


def source_rows(rows, x, f):
    put_pieces(rows, 0, f)
    put_pieces(rows, 3, f * (1.0 / 3.0))
    put_pieces(rows, 6, x)
    put_pieces(rows, 9, inner(f, x))
    put_pieces(rows, 10, inner(x, x) + BLOB)
    put(rows, 11, jnp.ones_like(x))


def target_rows(rows, x, f):
    a = f * KERNEL
    put_pieces(rows, 0, a)
    put_pieces(rows, 3, x)
    put_pieces(rows, 6, inner(a, x))
    put_pieces(rows, 7, inner(x, x))
    put(rows, 8, jnp.ones_like(x))


def flip(me, mask):
    bit = 1
    while bit <= mask:
        if mask & bit:
            me = me + bit - 2 * bit * lax.rem(lax.div(me, bit), 2)
        bit = 2 * bit
    return me


def split(n):
    bits = n.bit_length() - 1
    near = 1 << min(3, max(bits - 1, 0))
    return n // near, near


def body(
    n,
    near_src_hbm,
    near_count_hbm,
    far_count_hbm,
    pos_hbm,
    dens_hbm,
    far_slot_hbm,
    far_class_hbm,
    req_hbm,
    choose_src_hbm,
    choose_tgt_hbm,
    up_hbm,
    table_hbm,
    down_hbm,
    out,
    near_src,
    near_count,
    far_count,
    pos,
    dens,
    far_slot,
    far_class,
    req,
    choose_src,
    choose_tgt,
    pos_b,
    pos_a,
    dens_b,
    dens_a,
    up,
    table,
    down,
    dens_rows,
    mom,
    rows_own,
    rows_oth,
    window,
    rhs,
    lhs,
    tb,
    geo,
    tacc,
    cols,
    src_rows,
    hot_src,
    part_b,
    part_a,
    got_b,
    got_a,
    hot_class,
    hot_slot,
    ready,
    tiled,
    sums,
    fold,
    scatter,
    pick,
    spread,
    field,
    in_sem,
    up_sem,
    table_sem,
    down_sem,
    halo_send,
    halo_recv,
    mom_send,
    mom_recv,
    part_send,
    part_recv,
):
    leaves, width = mom.shape[1:]
    nodes = pos.shape[1]
    size = nodes // leaves
    slots = near_src.shape[0]
    far_num = far_slot.shape[1]
    classes = table.shape[0]
    cap = req.shape[0]
    block = fold.shape[0]
    outer, inner_n = split(n)
    expan_width = (width + 127) // 128 * 128
    me = lax.axis_index("patch")
    has_left = me > 0
    has_right = me < n - 1
    barrier = pltpu.get_barrier_semaphore()

    def signal(peer):
        pl.semaphore_signal(barrier, inc=1, device_id=(peer,), device_id_type=MESH)

    doublings = outer.bit_length() - 1
    for t in range(doublings):
        signal(flip(me, n >> (t + 1)))
    for k in range(1, inner_n):
        signal(flip(me, k))

    @pl.when(has_left)
    def _():
        signal(me - 1)

    @pl.when(has_right)
    def _():
        signal(me + 1)

    ins = [
        pltpu.make_async_copy(src, dst, in_sem.at[k])
        for k, (src, dst) in enumerate(
            (
                (pos_hbm, pos),
                (dens_hbm, dens),
                (choose_tgt_hbm, choose_tgt),
                (near_src_hbm, near_src),
                (near_count_hbm, near_count),
                (far_count_hbm, far_count),
                (far_slot_hbm, far_slot),
                (far_class_hbm, far_class),
                (req_hbm, req),
                (choose_src_hbm, choose_src),
            )
        )
    ]
    for copy in ins:
        copy.start()
    get_up = pltpu.make_async_copy(up_hbm, up, up_sem)
    get_up.start()

    def table_copy(b):
        lanes = pl.ds(pl.multiple_of(b * block, 128), block)
        return pltpu.make_async_copy(
            table_hbm.at[:, lanes], table.at[:, lanes], table_sem.at[b]
        )

    get_down = pltpu.make_async_copy(down_hbm, down, down_sem)
    for copy in ins:
        copy.wait()

    def halo(k, src, dst, peer):
        return pltpu.make_async_remote_copy(
            src_ref=src,
            dst_ref=dst,
            send_sem=halo_send.at[k],
            recv_sem=halo_recv.at[k],
            device_id=(peer,),
            device_id_type=MESH,
        )

    to_right = (halo(0, pos, pos_b, me + 1), halo(1, dens, dens_b, me + 1))
    to_left = (halo(2, pos, pos_a, me - 1), halo(3, dens, dens_a, me - 1))

    def gather(k, mask, first, count):
        return pltpu.make_async_remote_copy(
            src_ref=mom.at[0:count],
            dst_ref=mom.at[first : first + count],
            send_sem=mom_send.at[k],
            recv_sem=mom_recv.at[k],
            device_id=(flip(me, mask),),
            device_id_type=MESH,
        )

    far_step = [gather(t, n >> (t + 1), 1 << t, 1 << t) for t in range(doublings)]
    near_step = [
        gather(doublings - 1 + k, k, k * outer, outer) for k in range(1, inner_n)
    ]

    def sources(part, rows, x, f):
        source_rows(rows, x[...], f[...])
        for leaf in range(leaves):
            lanes = slice(leaf * size, (leaf + 1) * size)
            window[part * leaves + leaf, 0:3, :] = x[:, lanes] * 3.0
            window[part * leaves + leaf, 3:6, :] = f[:, lanes]

        for leaf in range(0, leaves, 2):
            chosen = dot(
                choose_src[...], rows[:, leaf * size : (leaf + 2) * size].astype(BF16)
            ).astype(BF16)
            for k in range(2):
                for o in range(4):
                    rhs[part * leaves + leaf + k, :, o * size : (o + 1) * size] = chosen[
                        o * FEATURES : (o + 1) * FEATURES, k * size : (k + 1) * size
                    ]

    rows_oth[...] = jnp.zeros_like(rows_oth)
    window[...] = jnp.zeros_like(window)
    nothing = jnp.zeros((3, size), F32)
    source_rows(rows_oth, nothing, nothing)
    chosen = dot(choose_src[...], rows_oth[:, :size].astype(BF16)).astype(BF16)
    for o in range(4):
        rhs[3 * leaves, :, o * size : (o + 1) * size] = chosen[
            o * FEATURES : (o + 1) * FEATURES
        ]
    sources(1, rows_oth, pos, dens)

    for leaf in range(leaves):
        for c in range(3):
            dens_rows[leaf : leaf + 1, c * size : (c + 1) * size] = dens[
                c : c + 1, leaf * size : (leaf + 1) * size
            ]
    dens_round = dens_rows[...].astype(BF16)
    get_up.wait()
    for b in range(width * width // block):
        table_copy(b).start()
    get_down.start()
    row = iota((leaves, width), 0)
    total = jnp.zeros((leaves, width), F32)
    for leaf in range(leaves):
        got = lax.dot_general(
            dens_round, up[leaf], (((1,), (1,)), ((), ())), preferred_element_type=F32
        )
        total = total + jnp.where(row == leaf, got, 0.0)
    mom[0] = total.astype(BF16)

    pl.semaphore_wait(
        barrier,
        doublings + inner_n - 1 + has_left.astype(jnp.int32) + has_right.astype(jnp.int32),
    )

    @pl.when(has_right)
    def _():
        for copy in to_right:
            copy.start()

    @pl.when(has_left)
    def _():
        for copy in to_left:
            copy.start()


    far_step[0].start()

    rows_own[...] = jnp.zeros_like(rows_own)
    target_rows(rows_own, pos[...], dens[...])

    few = 4

    for group in range(leaves // few):
        turned = []
        for k in range(few):
            start = pl.multiple_of((group * few + k) * size, size)
            turned.append(jnp.transpose(rows_own[:, pl.ds(start, size)]).astype(BF16))
        turned = jnp.concatenate(turned, axis=0)
        spread_out = dot(turned, choose_tgt[...])
        for k in range(few):
            mine = spread_out[k * size : (k + 1) * size]
            lhs[group * few + k] = mine[:, :128].astype(BF16)
            tb[group * few + k] = mine[:, 128:]

    count_col = jnp.zeros((leaves, 1), jnp.int32)
    leaf_col = iota((leaves, 1), 0)
    for leaf in range(leaves):
        count_col = jnp.where(leaf_col == leaf, far_count[leaf], count_col)
    class_iota = iota((leaves, classes), 1)
    column = iota((leaves, cap * n), 1)
    slot_of = lax.rem(column, n) * cap + lax.div(column, n)
    for s in range(far_num):
        rows = slice(s * leaves, (s + 1) * leaves)
        wanted = jnp.where(s < count_col, far_class[:, s : s + 1], -1)
        hot_class[rows, :] = (class_iota == wanted).astype(F32).astype(BF16)
        slot = far_slot[:, s : s + 1]
        hot_slot[rows, :] = (slot_of == slot).astype(F32).astype(BF16)
    fold_row = iota(fold.shape, 0)
    fold_first = iota(fold.shape, 1) * width
    fold[...] = (
        ((fold_row >= fold_first) & (fold_row < fold_first + width)).astype(F32).astype(BF16)
    )
    cols[...] = jnp.zeros_like(cols)
    offset = (me - 1) * leaves
    lane8 = iota((8, size), 1)
    lane1 = iota((1, 128), 1)

    def source_of(leaf, slot):
        live = slot < near_count[leaf]
        return jnp.where(live, near_src[slot, leaf] - offset, 3 * leaves)

    for leaf in range(leaves):
        for slot in range(slots):
            hot_src[leaf, slot : slot + 1, :] = (lane1 == source_of(leaf, slot)).astype(F32)
    scatter[...] = jnp.transpose(hot_src[...].reshape(leaves * slots, 128)).astype(BF16)

    device = iota((1, n), 1)
    place_of = jnp.zeros((1, n), jnp.int32)
    for t in range(n.bit_length() - 1):
        bit = 1 << t
        mine = lax.rem(lax.div(me, bit), 2)
        theirs = lax.rem(lax.div(device, bit), 2)
        place = bit * outer if bit < inner_n else n // (2 * bit)
        place_of = place_of + (theirs + mine - 2 * theirs * mine) * place
    row_iota = iota((n * leaves, n), 0)
    wanted = jnp.concatenate(
        [
            (row_iota == place_of * leaves + req[place : place + 1, :]).astype(F32)
            for place in range(cap)
        ],
        axis=1,
    )
    pick[...] = jnp.transpose(wanted).astype(BF16)
    period = tiled.shape[1]
    spread_gap = iota((width, period), 1) - iota((width, period), 0)
    near_gap = spread_gap == 0
    for k in range(1, period // width):
        near_gap = near_gap | (spread_gap == k * width)
    spread[...] = near_gap.astype(F32).astype(BF16)

    @pl.when(has_left)
    def _():
        for copy in to_right:
            copy.wait_recv()

    @pl.when(jnp.logical_not(has_left))
    def _():
        pos_b[...] = jnp.zeros_like(pos_b)
        dens_b[...] = jnp.zeros_like(dens_b)

    @pl.when(has_right)
    def _():
        for copy in to_left:
            copy.wait_recv()

    @pl.when(jnp.logical_not(has_right))
    def _():
        pos_a[...] = jnp.zeros_like(pos_a)
        dens_a[...] = jnp.zeros_like(dens_a)

    sources(0, rows_oth, pos_b, dens_b)
    sources(2, rows_own, pos_a, dens_a)

    together = 4
    ahead = 2
    halves = 1
    steps = together * slots
    turns = leaves // together

    def geometry(leaf, slot):
        return dot(lhs[leaf][:, :FEATURES], rhs[source_of(leaf, slot)])

    for k in range(ahead):
        geo[k][...] = geometry(0, k)

    step = 256 if block % 256 == 0 else 128
    per_block = block // width
    blocks = width * width // block
    early = ready.shape[0]
    share = early // turns
    jobs = [
        (k, t, h) for k in range(share) for t in range(block // step) for h in range(halves)
    ]

    @pl.loop(0, turns)
    def _(turn):
        for t in range(1, doublings):
            @pl.when(turn == min(t, turns // 2))
            def _(t=t):
                far_step[t - 1].wait_recv()
                far_step[t].start()

        @pl.when(turn == turns // 2)
        def _():
            far_step[-1].wait_recv()
            for copy in near_step:
                copy.start()

        for k in range(share):
            table_copy(turn * share + k).wait()
        held = [geo[k] for k in range(ahead)]
        for sub in range(steps):
            leaf = turn * together + sub // slots
            slot = sub % slots
            nxt = sub + ahead
            if nxt < steps:
                held.append(geometry(turn * together + nxt // slots, nxt % slots))
            else:
                after = lax.rem((turn + 1) * together + (nxt - steps) // slots, leaves)
                geo[nxt - steps][...] = geometry(after, (nxt - steps) % slots)
            for job in range(sub * len(jobs) // steps, (sub + 1) * len(jobs) // steps):
                k, t, h = jobs[job]
                start = pl.multiple_of((turn * share + k) * block + t * step, 128)
                rows = far_num * leaves // halves
                lines = slice(h * rows, (h + 1) * rows)
                ready[turn * share + k, lines, t * step : (t + 1) * step] = dot(
                    hot_class[lines, :], table[:, pl.ds(start, step)]
                )
            now = held[sub]
            nodes_k = window[source_of(leaf, slot)]
            xs = [jnp.broadcast_to(nodes_k[c : c + 1], (8, size)) for c in range(3)]
            fs = [jnp.broadcast_to(nodes_k[3 + c : 4 + c], (8, size)) for c in range(3)]
            sums_src = [None] * 3
            for g in range(size // 8):
                r8 = slice(g * 8, (g + 1) * 8)
                ab, ar, br, rho = [now[r8, o * size : (o + 1) * size] for o in range(4)]
                inv1 = lax.rsqrt(rho)
                inv2 = inv1 * inv1
                inv3 = inv1 * inv2
                p = br * inv3
                q = ar * inv3
                w = ab * inv3 + (p * ar) * inv2
                for c in range(3):
                    sep = tb[leaf, r8, c * size : (c + 1) * size] - xs[c]
                    a = tb[leaf, r8, (3 + c) * size : (4 + c) * size]
                    term = a * p + fs[c] * q - w * sep
                    sums_src[c] = term if g == 0 else sums_src[c] + term
                    total = term if slot == 0 else term + tacc[c, r8, :]
                    if slot + 1 < slots:
                        tacc[c, r8, :] = total
                    else:
                        col = jnp.sum(total, axis=1, keepdims=True)
                        cols[r8, :] = jnp.where(lane8 == c * leaves + leaf, col, cols[r8, :])
            for c in range(3):
                src_rows[leaf, slot : slot + 1, c * size : (c + 1) * size] = jnp.sum(
                    sums_src[c], axis=0, keepdims=True
                )

    for copy in near_step:
        copy.wait_recv()

    near_t = jnp.transpose(cols[...])
    values = src_rows[...].reshape(leaves * slots, 3 * size)
    scattered = None
    for piece in pieces(values):
        term = dot(scatter[...], piece.astype(BF16))
        scattered = term if scattered is None else scattered + term
    part_b[...] = scattered[:leaves]
    part_a[...] = scattered[2 * leaves : 3 * leaves]
    own = scattered[leaves : 2 * leaves]
    near = [
        near_t[c * leaves : (c + 1) * leaves] - own[:, c * size : (c + 1) * size]
        for c in range(3)
    ]
    for c in range(3):
        field[9 + c] = near[c]

    def part(k, src, dst, peer):
        return pltpu.make_async_remote_copy(
            src_ref=src,
            dst_ref=dst,
            send_sem=part_send.at[k],
            recv_sem=part_recv.at[k],
            device_id=(peer,),
            device_id_type=MESH,
        )

    part_left = part(0, part_b, got_a, me - 1)
    part_right = part(1, part_a, got_b, me + 1)

    @pl.when(has_left)
    def _():
        part_left.start()

    @pl.when(has_right)
    def _():
        part_right.start()

    moments = mom[...].reshape(n * leaves, width)
    chosen = dot(pick[...], moments).astype(BF16)
    chosen_rows = dot(chosen, spread[...]).astype(BF16)
    tiled[...] = dot(hot_slot[...], chosen_rows)


    def apply(members, t):
        for h in range(step // 128):
            tile = ((t * step) // 128 + h) % (period // 128)
            acc = [None] * len(members)
            for s in range(far_num):
                rows = slice(s * leaves, (s + 1) * leaves)
                factor = tiled[rows, tile * 128 : (tile + 1) * 128]
                for k, (b, oper) in enumerate(members):
                    term = oper(rows, h) * factor
                    acc[k] = term if acc[k] is None else acc[k] + term
            for k, (b, oper) in enumerate(members):
                lines = pl.ds(pl.multiple_of(b * leaves, leaves), leaves)
                sums[lines, t * step + h * 128 : t * step + (h + 1) * 128] = acc[k]

    def fresh(b, t):
        start = pl.multiple_of(b * block + t * step, 128)
        oper = dot(hot_class[...], table[:, pl.ds(start, step)])
        return b, lambda rows, h: oper[rows, h * 128 : (h + 1) * 128]

    def stored(b, t):
        return b, lambda rows, h: ready[
            b, rows, t * step + h * 128 : t * step + (h + 1) * 128
        ]

    paired = min(early, blocks - early)

    @pl.loop(0, paired)
    def _(b):
        table_copy(early + b).wait()
        for t in range(block // step):
            apply((fresh(early + b, t), stored(b, t)), t)

    for b in range(early + paired, blocks):
        table_copy(b).wait()
        for t in range(block // step):
            apply((fresh(b, t),), t)

    whole = sums[...]
    high = whole.astype(BF16)
    low = (whole - high.astype(F32)).astype(BF16)
    res = dot(high, fold[...]) + dot(low, fold[...])
    wide = jnp.zeros((leaves, expan_width), F32)
    for b in range(blocks):
        one = jnp.concatenate(
            [res[b * leaves : (b + 1) * leaves], jnp.zeros((leaves, expan_width - 128), F32)], axis=1
        )
        wide = wide + (pltpu.roll(one, b * per_block, 1) if b else one)
    expansion = wide[:, :width]
    get_down.wait()
    leaf_row = iota((leaves, width), 0)
    nothing = jnp.zeros_like(expansion)
    single = [
        jnp.where(leaf_row == leaf, expansion, nothing).astype(BF16) for leaf in range(leaves)
    ]
    for q in range(9):
        total = None
        for leaf in range(leaves):
            got = dot(single[leaf], down[leaf, q])
            total = got if total is None else total + got
        field[q] = total

    @pl.when(has_right)
    def _():
        part_left.wait_recv()

    @pl.when(jnp.logical_not(has_right))
    def _():
        got_a[...] = jnp.zeros_like(got_a)

    @pl.when(has_left)
    def _():
        part_right.wait_recv()

    @pl.when(jnp.logical_not(has_left))
    def _():
        got_b[...] = jnp.zeros_like(got_b)

    for k in range(3):
        lanes = slice(k * size, (k + 1) * size)
        result = field[9 + k] - (got_b[:, lanes] + got_a[:, lanes])
        for c in range(3):
            result = result + dens_rows[:, c * size : (c + 1) * size] * field[3 * c + k]
        for leaf in range(leaves):
            out[k : k + 1, leaf * size : (leaf + 1) * size] = result[leaf : leaf + 1]

    @pl.when(has_right)
    def _():
        part_right.wait_send()
        for copy in to_right:
            copy.wait_send()

    @pl.when(has_left)
    def _():
        part_left.wait_send()
        for copy in to_left:
            copy.wait_send()

    for copy in far_step + near_step:
        copy.wait_send()


def per_device(
    n,
    positions,
    densities,
    near_src,
    near_count,
    far_slot,
    far_class,
    far_count,
    requests,
    up_basis,
    transfer_table,
    down_basis,
):
    leaves, slots = near_src.shape
    nodes = positions.shape[1]
    size = nodes // leaves
    width = up_basis.shape[1]
    far_num = far_slot.shape[1]
    cap = requests.shape[2]
    classes = transfer_table.shape[0]
    copies = split(n)[0].bit_length() + split(n)[1] - 2
    period = math.lcm(width, 128)
    blocks = width * width // period
    block = 2 * period if blocks % 2 == 0 else period
    down = jnp.transpose(down_basis, (0, 2, 1, 3))
    blocks = width * width // block
    vmem = pl.BlockSpec(memory_space=pltpu.VMEM)
    hbm = pl.BlockSpec(memory_space=pl.ANY)
    line = pltpu.VMEM((3, nodes), F32)
    part = pltpu.VMEM((leaves, 3 * size), F32)
    return pl.pallas_call(
        functools.partial(body, n),
        out_shape=pltpu.VMEM((3, nodes), F32),
        in_specs=[hbm] * 13,
        out_specs=vmem,
        scratch_shapes=[
            pltpu.SMEM((slots, leaves), jnp.int32),
            pltpu.SMEM((leaves,), jnp.int32),
            pltpu.SMEM((leaves,), jnp.int32),
            line,
            line,
            pltpu.VMEM(far_slot.shape, jnp.int32),
            pltpu.VMEM(far_class.shape, jnp.int32),
            pltpu.VMEM((cap, n), jnp.int32),
            pltpu.VMEM((4 * FEATURES, ROWS), BF16),
            pltpu.VMEM((ROWS, 128 + 6 * size), BF16),
        ]
        + [line] * 4
        + [
            pltpu.VMEM(up_basis.shape, BF16),
            pltpu.VMEM(transfer_table.shape, BF16),
            pltpu.VMEM(down.shape, BF16),
            part,
            pltpu.VMEM((n, leaves, width), BF16),
            pltpu.VMEM((ROWS, nodes), F32),
            pltpu.VMEM((ROWS, nodes), F32),
            pltpu.VMEM((3 * leaves + 1, 8, size), F32),
            pltpu.VMEM((3 * leaves + 1, FEATURES, 4 * size), BF16),
            pltpu.VMEM((leaves, size, 128), BF16),
            pltpu.VMEM((leaves, size, 6 * size), F32),
            [pltpu.VMEM((size, 4 * size), F32)] * 2,
            pltpu.VMEM((3, size, size), F32),
            pltpu.VMEM((size, 128), F32),
            pltpu.VMEM((leaves, slots, 3 * size), F32),
            pltpu.VMEM((leaves, slots, 128), F32),
            part,
            part,
            part,
            part,
            pltpu.VMEM((far_num * leaves, classes), BF16),
            pltpu.VMEM((far_num * leaves, cap * n), BF16),
            pltpu.VMEM((4, far_num * leaves, block), F32),
            pltpu.VMEM((far_num * leaves, period), F32),
            pltpu.VMEM((blocks * leaves, block), F32),
            pltpu.VMEM((block, 128), BF16),
            pltpu.VMEM((128, leaves * slots), BF16),
            pltpu.VMEM((cap * n, n * leaves), BF16),
            pltpu.VMEM((width, period), BF16),
            pltpu.VMEM((12, leaves, size), F32),
            pltpu.SemaphoreType.DMA((10,)),
            pltpu.SemaphoreType.DMA,
            pltpu.SemaphoreType.DMA((blocks,)),
            pltpu.SemaphoreType.DMA,
            pltpu.SemaphoreType.DMA((4,)),
            pltpu.SemaphoreType.DMA((4,)),
            pltpu.SemaphoreType.DMA((copies,)),
            pltpu.SemaphoreType.DMA((copies,)),
            pltpu.SemaphoreType.DMA((2,)),
            pltpu.SemaphoreType.DMA((2,)),
        ],
        compiler_params=pltpu.CompilerParams(
            collective_id=0,
            has_side_effects=True,
            vmem_limit_bytes=60 * 1024 * 1024,
        ),
    )(
        near_src.T,
        near_count,
        far_count,
        positions,
        densities,
        far_slot,
        far_class,
        requests[0].T,
        jnp.asarray(source_choice(), BF16),
        jnp.asarray(target_choice(size), BF16),
        up_basis,
        transfer_table,
        down,
    )


def solution(mesh):
    placed = (
        P(None, "patch"),
        P(None, "patch"),
        P("patch", None),
        P("patch"),
        P("patch", None),
        P("patch", None),
        P("patch"),
        P("patch", None, None),
        P("patch", None, None),
        P(),
        P("patch", None, None, None),
    )
    return jax.shard_map(
        functools.partial(per_device, mesh.shape["patch"]),
        mesh=mesh,
        in_specs=placed,
        out_specs=P(None, "patch"),
        check_vma=False,
    )
```

```python
import functools
import math

import jax
import jax.numpy as jnp
import numpy as np
from jax import lax
from jax.experimental import pallas as pl
from jax.experimental.pallas import tpu as pltpu
from jax.sharding import PartitionSpec as P

KERNEL = 1.0 / (8.0 * math.pi)
BLOB = 0.25
MESH = pl.DeviceIdType.MESH
F32 = jnp.float32
BF16 = jnp.bfloat16

ROWS = 48
FEATURES = 48
LEFT = (0, 0, 0, 1, 1, 2)
RIGHT = (0, 1, 2, 0, 1, 0)


def at(group):
    return (group // 2) * 8 + (group % 2) * 3


def source_choice():
    sel = np.zeros((4, FEATURES, ROWS), np.float32)
    for k in range(6):
        for c in range(3):
            sel[0, 3 * k + c, at(3 + RIGHT[k]) + c] = 1.0
            sel[1, 3 * k + c, at(6 + RIGHT[k]) + c] = -1.0
            sel[2, 18 + 3 * k + c, at(RIGHT[k]) + c] = 1.0
            sel[3, 18 + 3 * k + c, at(6 + RIGHT[k]) + c] = -2.0
    for c in range(3):
        sel[1, 36 + c, at(11) + c] = 1.0
        sel[2, 42 + c, at(9) + c] = -1.0
        sel[3, 39 + c, at(11) + c] = 1.0
        sel[3, 42 + c, at(10) + c] = 1.0
    return sel.reshape(4 * FEATURES, ROWS)


def target_choice(size):
    sel = np.zeros((ROWS, 128), np.float32)
    spread = np.zeros((ROWS, 6, size), np.float32)
    for k in range(6):
        for c in range(3):
            sel[at(LEFT[k]) + c, 3 * k + c] = 1.0
            sel[at(3 + LEFT[k]) + c, 18 + 3 * k + c] = 1.0
    for c in range(3):
        sel[at(6) + c, 36 + c] = 1.0
        sel[at(7) + c, 39 + c] = 1.0
        sel[at(8) + c, 42 + c] = 1.0
        for piece in range(3):
            spread[at(3 + piece) + c, c, :] = 3.0
            spread[at(piece) + c, 3 + c, :] = 1.0
    return np.concatenate([sel, spread.reshape(ROWS, 6 * size)], axis=1)


def iota(shape, dim):
    return lax.broadcasted_iota(jnp.int32, shape, dim)


def dot(a, b):
    return jnp.dot(a, b, preferred_element_type=F32)


def pieces(x):
    high = x.astype(BF16).astype(F32)
    rest = x - high
    mid = rest.astype(BF16).astype(F32)
    return high, mid, rest - mid


def inner(a, b):
    return a[0:1] * b[0:1] + a[1:2] * b[1:2] + a[2:3] * b[2:3]


def put(rows, group, value):
    rows[at(group) : at(group) + value.shape[0], : value.shape[1]] = value


def put_pieces(rows, group, value):
    for k, piece in enumerate(pieces(value)):
        if value.shape[0] == 3:
            put(rows, group + k, piece)
        else:
            rows[at(group) + k : at(group) + k + 1, : value.shape[1]] = piece


def source_rows(rows, x, f):
    put_pieces(rows, 0, f)
    put_pieces(rows, 3, f * (1.0 / 3.0))
    put_pieces(rows, 6, x)
    put_pieces(rows, 9, inner(f, x))
    put_pieces(rows, 10, inner(x, x) + BLOB)
    put(rows, 11, jnp.ones_like(x))


def target_rows(rows, x, f):
    a = f * KERNEL
    put_pieces(rows, 0, a)
    put_pieces(rows, 3, x)
    put_pieces(rows, 6, inner(a, x))
    put_pieces(rows, 7, inner(x, x))
    put(rows, 8, jnp.ones_like(x))


def flip(me, mask):
    bit = 1
    while bit <= mask:
        if mask & bit:
            me = me + bit - 2 * bit * lax.rem(lax.div(me, bit), 2)
        bit = 2 * bit
    return me


def split(n):
    bits = n.bit_length() - 1
    near = 1 << min(4, max(bits - 1, 0))
    return n // near, near


def body(
    n,
    near_src_hbm,
    near_count_hbm,
    far_count_hbm,
    pos_hbm,
    dens_hbm,
    far_slot_hbm,
    far_class_hbm,
    req_hbm,
    choose_src_hbm,
    choose_tgt_hbm,
    up_hbm,
    table_hbm,
    down_hbm,
    out,
    near_src,
    near_count,
    far_count,
    pos,
    dens,
    far_slot,
    far_class,
    req,
    choose_src,
    choose_tgt,
    pos_b,
    pos_a,
    dens_b,
    dens_a,
    up,
    table,
    down,
    dens_rows,
    mom,
    rows_own,
    rows_oth,
    window,
    rhs,
    lhs,
    tb,
    geo,
    tacc,
    cols,
    src_rows,
    hot_src,
    part_b,
    part_a,
    got_b,
    got_a,
    hot_class,
    hot_slot,
    ready,
    tiled,
    sums,
    fold,
    scatter,
    pick,
    spread,
    field,
    in_sem,
    up_sem,
    table_sem,
    down_sem,
    halo_send,
    halo_recv,
    mom_send,
    mom_recv,
    part_send,
    part_recv,
):
    leaves, width = mom.shape[1:]
    nodes = pos.shape[1]
    size = nodes // leaves
    slots = near_src.shape[0]
    far_num = far_slot.shape[1]
    classes = table.shape[0]
    cap = req.shape[0]
    block = fold.shape[0]
    outer, inner_n = split(n)
    expan_width = (width + 127) // 128 * 128
    me = lax.axis_index("patch")
    has_left = me > 0
    has_right = me < n - 1
    barrier = pltpu.get_barrier_semaphore()

    def signal(peer):
        pl.semaphore_signal(barrier, inc=1, device_id=(peer,), device_id_type=MESH)

    doublings = outer.bit_length() - 1
    for t in range(doublings):
        signal(flip(me, n >> (t + 1)))
    for k in range(1, inner_n):
        signal(flip(me, k))

    @pl.when(has_left)
    def _():
        signal(me - 1)

    @pl.when(has_right)
    def _():
        signal(me + 1)

    ins = [
        pltpu.make_async_copy(src, dst, in_sem.at[k])
        for k, (src, dst) in enumerate(
            (
                (pos_hbm, pos),
                (dens_hbm, dens),
                (choose_tgt_hbm, choose_tgt),
                (near_src_hbm, near_src),
                (near_count_hbm, near_count),
                (far_count_hbm, far_count),
                (far_slot_hbm, far_slot),
                (far_class_hbm, far_class),
                (req_hbm, req),
                (choose_src_hbm, choose_src),
            )
        )
    ]
    for copy in ins:
        copy.start()
    get_up = pltpu.make_async_copy(up_hbm, up, up_sem)
    get_up.start()

    def table_copy(b):
        lanes = pl.ds(pl.multiple_of(b * block, 128), block)
        return pltpu.make_async_copy(
            table_hbm.at[:, lanes], table.at[:, lanes], table_sem.at[b]
        )

    get_down = pltpu.make_async_copy(down_hbm, down, down_sem)
    for copy in ins:
        copy.wait()

    def halo(k, src, dst, peer):
        return pltpu.make_async_remote_copy(
            src_ref=src,
            dst_ref=dst,
            send_sem=halo_send.at[k],
            recv_sem=halo_recv.at[k],
            device_id=(peer,),
            device_id_type=MESH,
        )

    to_right = (halo(0, pos, pos_b, me + 1), halo(1, dens, dens_b, me + 1))
    to_left = (halo(2, pos, pos_a, me - 1), halo(3, dens, dens_a, me - 1))

    def gather(k, mask, first, count):
        return pltpu.make_async_remote_copy(
            src_ref=mom.at[0:count],
            dst_ref=mom.at[first : first + count],
            send_sem=mom_send.at[k],
            recv_sem=mom_recv.at[k],
            device_id=(flip(me, mask),),
            device_id_type=MESH,
        )

    far_step = [gather(t, n >> (t + 1), 1 << t, 1 << t) for t in range(doublings)]
    near_step = [
        gather(doublings - 1 + k, k, k * outer, outer) for k in range(1, inner_n)
    ]

    def sources(part, rows, x, f):
        source_rows(rows, x[...], f[...])
        for leaf in range(leaves):
            lanes = slice(leaf * size, (leaf + 1) * size)
            window[part * leaves + leaf, 0:3, :] = x[:, lanes] * 3.0
            window[part * leaves + leaf, 3:6, :] = f[:, lanes]

        for leaf in range(0, leaves, 2):
            chosen = dot(
                choose_src[...], rows[:, leaf * size : (leaf + 2) * size].astype(BF16)
            ).astype(BF16)
            for k in range(2):
                for o in range(4):
                    rhs[part * leaves + leaf + k, :, o * size : (o + 1) * size] = chosen[
                        o * FEATURES : (o + 1) * FEATURES, k * size : (k + 1) * size
                    ]

    rows_oth[...] = jnp.zeros_like(rows_oth)
    window[...] = jnp.zeros_like(window)
    nothing = jnp.zeros((3, size), F32)
    source_rows(rows_oth, nothing, nothing)
    chosen = dot(choose_src[...], rows_oth[:, :size].astype(BF16)).astype(BF16)
    for o in range(4):
        rhs[3 * leaves, :, o * size : (o + 1) * size] = chosen[
            o * FEATURES : (o + 1) * FEATURES
        ]
    sources(1, rows_oth, pos, dens)

    for leaf in range(leaves):
        for c in range(3):
            dens_rows[leaf : leaf + 1, c * size : (c + 1) * size] = dens[
                c : c + 1, leaf * size : (leaf + 1) * size
            ]
    dens_round = dens_rows[...].astype(BF16)
    get_up.wait()
    for b in range(width * width // block):
        table_copy(b).start()
    get_down.start()
    row = iota((leaves, width), 0)
    total = jnp.zeros((leaves, width), F32)
    for leaf in range(leaves):
        got = lax.dot_general(
            dens_round, up[leaf], (((1,), (1,)), ((), ())), preferred_element_type=F32
        )
        total = total + jnp.where(row == leaf, got, 0.0)
    mom[0] = total.astype(BF16)

    pl.semaphore_wait(
        barrier,
        doublings + inner_n - 1 + has_left.astype(jnp.int32) + has_right.astype(jnp.int32),
    )

    @pl.when(has_right)
    def _():
        for copy in to_right:
            copy.start()

    @pl.when(has_left)
    def _():
        for copy in to_left:
            copy.start()


    far_step[0].start()

    rows_own[...] = jnp.zeros_like(rows_own)
    target_rows(rows_own, pos[...], dens[...])

    few = 4

    for group in range(leaves // few):
        turned = []
        for k in range(few):
            start = pl.multiple_of((group * few + k) * size, size)
            turned.append(jnp.transpose(rows_own[:, pl.ds(start, size)]).astype(BF16))
        turned = jnp.concatenate(turned, axis=0)
        spread_out = dot(turned, choose_tgt[...])
        for k in range(few):
            mine = spread_out[k * size : (k + 1) * size]
            lhs[group * few + k] = mine[:, :128].astype(BF16)
            tb[group * few + k] = mine[:, 128:]

    count_col = jnp.zeros((leaves, 1), jnp.int32)
    leaf_col = iota((leaves, 1), 0)
    for leaf in range(leaves):
        count_col = jnp.where(leaf_col == leaf, far_count[leaf], count_col)
    class_iota = iota((leaves, classes), 1)
    column = iota((leaves, cap * n), 1)
    slot_of = lax.rem(column, n) * cap + lax.div(column, n)
    for s in range(far_num):
        rows = slice(s * leaves, (s + 1) * leaves)
        wanted = jnp.where(s < count_col, far_class[:, s : s + 1], -1)
        hot_class[rows, :] = (class_iota == wanted).astype(F32).astype(BF16)
        slot = far_slot[:, s : s + 1]
        hot_slot[rows, :] = (slot_of == slot).astype(F32).astype(BF16)
    fold_row = iota(fold.shape, 0)
    fold_first = iota(fold.shape, 1) * width
    fold[...] = (
        ((fold_row >= fold_first) & (fold_row < fold_first + width)).astype(F32).astype(BF16)
    )
    cols[...] = jnp.zeros_like(cols)
    offset = (me - 1) * leaves
    lane8 = iota((8, size), 1)
    lane1 = iota((1, 128), 1)

    def source_of(leaf, slot):
        live = slot < near_count[leaf]
        return jnp.where(live, near_src[slot, leaf] - offset, 3 * leaves)

    for leaf in range(leaves):
        for slot in range(slots):
            hot_src[leaf, slot : slot + 1, :] = (lane1 == source_of(leaf, slot)).astype(F32)
    scatter[...] = jnp.transpose(hot_src[...].reshape(leaves * slots, 128)).astype(BF16)

    device = iota((1, n), 1)
    place_of = jnp.zeros((1, n), jnp.int32)
    for t in range(n.bit_length() - 1):
        bit = 1 << t
        mine = lax.rem(lax.div(me, bit), 2)
        theirs = lax.rem(lax.div(device, bit), 2)
        place = bit * outer if bit < inner_n else n // (2 * bit)
        place_of = place_of + (theirs + mine - 2 * theirs * mine) * place
    row_iota = iota((n * leaves, n), 0)
    wanted = jnp.concatenate(
        [
            (row_iota == place_of * leaves + req[place : place + 1, :]).astype(F32)
            for place in range(cap)
        ],
        axis=1,
    )
    pick[...] = jnp.transpose(wanted).astype(BF16)
    period = tiled.shape[1]
    spread_gap = iota((width, period), 1) - iota((width, period), 0)
    near_gap = spread_gap == 0
    for k in range(1, period // width):
        near_gap = near_gap | (spread_gap == k * width)
    spread[...] = near_gap.astype(F32).astype(BF16)

    @pl.when(has_left)
    def _():
        for copy in to_right:
            copy.wait_recv()

    @pl.when(jnp.logical_not(has_left))
    def _():
        pos_b[...] = jnp.zeros_like(pos_b)
        dens_b[...] = jnp.zeros_like(dens_b)

    @pl.when(has_right)
    def _():
        for copy in to_left:
            copy.wait_recv()

    @pl.when(jnp.logical_not(has_right))
    def _():
        pos_a[...] = jnp.zeros_like(pos_a)
        dens_a[...] = jnp.zeros_like(dens_a)

    sources(0, rows_oth, pos_b, dens_b)
    sources(2, rows_own, pos_a, dens_a)

    together = 4
    ahead = 2
    halves = 1
    steps = together * slots
    turns = leaves // together

    def geometry(leaf, slot):
        return dot(lhs[leaf][:, :FEATURES], rhs[source_of(leaf, slot)])

    for k in range(ahead):
        geo[k][...] = geometry(0, k)

    step = 256 if block % 256 == 0 else 128
    per_block = block // width
    blocks = width * width // block
    early = ready.shape[0]
    share = early // turns
    jobs = [
        (k, t, h) for k in range(share) for t in range(block // step) for h in range(halves)
    ]

    @pl.loop(0, turns)
    def _(turn):
        for t in range(1, doublings):
            @pl.when(turn == min(t, turns // 2))
            def _(t=t):
                far_step[t - 1].wait_recv()
                far_step[t].start()

        @pl.when(turn == min(doublings, turns // 2))
        def _():
            far_step[-1].wait_recv()
            for copy in near_step:
                copy.start()

        for k in range(share):
            table_copy(turn * share + k).wait()
        held = [geo[k] for k in range(ahead)]
        for sub in range(steps):
            leaf = turn * together + sub // slots
            slot = sub % slots
            nxt = sub + ahead
            if nxt < steps:
                held.append(geometry(turn * together + nxt // slots, nxt % slots))
            else:
                after = lax.rem((turn + 1) * together + (nxt - steps) // slots, leaves)
                geo[nxt - steps][...] = geometry(after, (nxt - steps) % slots)
            for job in range(sub * len(jobs) // steps, (sub + 1) * len(jobs) // steps):
                k, t, h = jobs[job]
                start = pl.multiple_of((turn * share + k) * block + t * step, 128)
                rows = far_num * leaves // halves
                lines = slice(h * rows, (h + 1) * rows)
                ready[turn * share + k, lines, t * step : (t + 1) * step] = dot(
                    hot_class[lines, :], table[:, pl.ds(start, step)]
                )
            now = held[sub]
            nodes_k = window[source_of(leaf, slot)]
            xs = [jnp.broadcast_to(nodes_k[c : c + 1], (8, size)) for c in range(3)]
            fs = [jnp.broadcast_to(nodes_k[3 + c : 4 + c], (8, size)) for c in range(3)]
            sums_src = [None] * 3
            for g in range(size // 8):
                r8 = slice(g * 8, (g + 1) * 8)
                ab, ar, br, rho = [now[r8, o * size : (o + 1) * size] for o in range(4)]
                inv1 = lax.rsqrt(rho)
                inv2 = inv1 * inv1
                inv3 = inv1 * inv2
                p = br * inv3
                q = ar * inv3
                w = ab * inv3 + (p * ar) * inv2
                for c in range(3):
                    sep = tb[leaf, r8, c * size : (c + 1) * size] - xs[c]
                    a = tb[leaf, r8, (3 + c) * size : (4 + c) * size]
                    term = a * p + fs[c] * q - w * sep
                    sums_src[c] = term if g == 0 else sums_src[c] + term
                    total = term if slot == 0 else term + tacc[c, r8, :]
                    if slot + 1 < slots:
                        tacc[c, r8, :] = total
                    else:
                        col = jnp.sum(total, axis=1, keepdims=True)
                        cols[r8, :] = jnp.where(lane8 == c * leaves + leaf, col, cols[r8, :])
            for c in range(3):
                src_rows[leaf, slot : slot + 1, c * size : (c + 1) * size] = jnp.sum(
                    sums_src[c], axis=0, keepdims=True
                )

    for copy in near_step:
        copy.wait_recv()

    near_t = jnp.transpose(cols[...])
    values = src_rows[...].reshape(leaves * slots, 3 * size)
    scattered = None
    for piece in pieces(values):
        term = dot(scatter[...], piece.astype(BF16))
        scattered = term if scattered is None else scattered + term
    part_b[...] = scattered[:leaves]
    part_a[...] = scattered[2 * leaves : 3 * leaves]
    own = scattered[leaves : 2 * leaves]
    near = [
        near_t[c * leaves : (c + 1) * leaves] - own[:, c * size : (c + 1) * size]
        for c in range(3)
    ]
    for c in range(3):
        field[9 + c] = near[c]

    def part(k, src, dst, peer):
        return pltpu.make_async_remote_copy(
            src_ref=src,
            dst_ref=dst,
            send_sem=part_send.at[k],
            recv_sem=part_recv.at[k],
            device_id=(peer,),
            device_id_type=MESH,
        )

    part_left = part(0, part_b, got_a, me - 1)
    part_right = part(1, part_a, got_b, me + 1)

    @pl.when(has_left)
    def _():
        part_left.start()

    @pl.when(has_right)
    def _():
        part_right.start()

    moments = mom[...].reshape(n * leaves, width)
    chosen = dot(pick[...], moments).astype(BF16)
    chosen_rows = dot(chosen, spread[...]).astype(BF16)
    tiled[...] = dot(hot_slot[...], chosen_rows)


    def apply(members, t):
        for h in range(step // 128):
            tile = ((t * step) // 128 + h) % (period // 128)
            acc = [None] * len(members)
            for s in range(far_num):
                rows = slice(s * leaves, (s + 1) * leaves)
                factor = tiled[rows, tile * 128 : (tile + 1) * 128]
                for k, (b, oper) in enumerate(members):
                    term = oper(rows, h) * factor
                    acc[k] = term if acc[k] is None else acc[k] + term
            for k, (b, oper) in enumerate(members):
                lines = pl.ds(pl.multiple_of(b * leaves, leaves), leaves)
                sums[lines, t * step + h * 128 : t * step + (h + 1) * 128] = acc[k]

    def fresh(b, t):
        start = pl.multiple_of(b * block + t * step, 128)
        oper = dot(hot_class[...], table[:, pl.ds(start, step)])
        return b, lambda rows, h: oper[rows, h * 128 : (h + 1) * 128]

    def stored(b, t):
        return b, lambda rows, h: ready[
            b, rows, t * step + h * 128 : t * step + (h + 1) * 128
        ]

    paired = min(early, blocks - early)

    @pl.loop(0, paired // 2)
    def _(turn):
        for k in range(2):
            table_copy(early + turn * 2 + k).wait()
        for k in range(2):
            b = turn * 2 + k
            for t in range(block // step):
                apply((fresh(early + b, t), stored(b, t)), t)

    for b in range(early + paired, blocks):
        table_copy(b).wait()
        for t in range(block // step):
            apply((fresh(b, t),), t)

    whole = sums[...]
    high = whole.astype(BF16)
    low = (whole - high.astype(F32)).astype(BF16)
    res = dot(high, fold[...]) + dot(low, fold[...])
    wide = jnp.zeros((leaves, expan_width), F32)
    for b in range(blocks):
        one = jnp.concatenate(
            [res[b * leaves : (b + 1) * leaves], jnp.zeros((leaves, expan_width - 128), F32)], axis=1
        )
        wide = wide + (pltpu.roll(one, b * per_block, 1) if b else one)
    expansion = wide[:, :width]
    get_down.wait()
    leaf_row = iota((leaves, width), 0)
    nothing = jnp.zeros_like(expansion)
    single = [
        jnp.where(leaf_row == leaf, expansion, nothing).astype(BF16) for leaf in range(leaves)
    ]
    on_vpu = 3
    for q in range(9 - on_vpu):
        total = None
        for leaf in range(leaves):
            got = dot(single[leaf], down[leaf, q])
            total = got if total is None else total + got
        field[q] = total
    padded = jnp.concatenate([wide, jnp.zeros((128 - leaves, expan_width), F32)], axis=0)
    turned = jnp.transpose(padded.astype(BF16).astype(F32))[:width]
    for leaf in range(leaves):
        column = jnp.broadcast_to(turned[:, leaf : leaf + 1], (width, size))
        for q in range(9 - on_vpu, 9):
            product = column * down[leaf, q].astype(F32)
            field[q, leaf : leaf + 1, :] = jnp.sum(product, axis=0, keepdims=True)

    @pl.when(has_right)
    def _():
        part_left.wait_recv()

    @pl.when(jnp.logical_not(has_right))
    def _():
        got_a[...] = jnp.zeros_like(got_a)

    @pl.when(has_left)
    def _():
        part_right.wait_recv()

    @pl.when(jnp.logical_not(has_left))
    def _():
        got_b[...] = jnp.zeros_like(got_b)

    for k in range(3):
        lanes = slice(k * size, (k + 1) * size)
        result = field[9 + k] - (got_b[:, lanes] + got_a[:, lanes])
        for c in range(3):
            result = result + dens_rows[:, c * size : (c + 1) * size] * field[3 * c + k]
        for leaf in range(leaves):
            out[k : k + 1, leaf * size : (leaf + 1) * size] = result[leaf : leaf + 1]

    @pl.when(has_right)
    def _():
        part_right.wait_send()
        for copy in to_right:
            copy.wait_send()

    @pl.when(has_left)
    def _():
        part_left.wait_send()
        for copy in to_left:
            copy.wait_send()

    for copy in far_step + near_step:
        copy.wait_send()


def per_device(
    n,
    positions,
    densities,
    near_src,
    near_count,
    far_slot,
    far_class,
    far_count,
    requests,
    up_basis,
    transfer_table,
    down_basis,
):
    leaves, slots = near_src.shape
    nodes = positions.shape[1]
    size = nodes // leaves
    width = up_basis.shape[1]
    far_num = far_slot.shape[1]
    cap = requests.shape[2]
    classes = transfer_table.shape[0]
    copies = split(n)[0].bit_length() + split(n)[1] - 2
    period = math.lcm(width, 128)
    blocks = width * width // period
    block = 2 * period if blocks % 2 == 0 else period
    down = jnp.transpose(down_basis, (0, 2, 1, 3))
    blocks = width * width // block
    vmem = pl.BlockSpec(memory_space=pltpu.VMEM)
    hbm = pl.BlockSpec(memory_space=pl.ANY)
    line = pltpu.VMEM((3, nodes), F32)
    part = pltpu.VMEM((leaves, 3 * size), F32)
    return pl.pallas_call(
        functools.partial(body, n),
        out_shape=pltpu.VMEM((3, nodes), F32),
        in_specs=[hbm] * 13,
        out_specs=vmem,
        scratch_shapes=[
            pltpu.SMEM((slots, leaves), jnp.int32),
            pltpu.SMEM((leaves,), jnp.int32),
            pltpu.SMEM((leaves,), jnp.int32),
            line,
            line,
            pltpu.VMEM(far_slot.shape, jnp.int32),
            pltpu.VMEM(far_class.shape, jnp.int32),
            pltpu.VMEM((cap, n), jnp.int32),
            pltpu.VMEM((4 * FEATURES, ROWS), BF16),
            pltpu.VMEM((ROWS, 128 + 6 * size), BF16),
        ]
        + [line] * 4
        + [
            pltpu.VMEM(up_basis.shape, BF16),
            pltpu.VMEM(transfer_table.shape, BF16),
            pltpu.VMEM(down.shape, BF16),
            part,
            pltpu.VMEM((n, leaves, width), BF16),
            pltpu.VMEM((ROWS, nodes), F32),
            pltpu.VMEM((ROWS, nodes), F32),
            pltpu.VMEM((3 * leaves + 1, 8, size), F32),
            pltpu.VMEM((3 * leaves + 1, FEATURES, 4 * size), BF16),
            pltpu.VMEM((leaves, size, 128), BF16),
            pltpu.VMEM((leaves, size, 6 * size), F32),
            [pltpu.VMEM((size, 4 * size), F32)] * 2,
            pltpu.VMEM((3, size, size), F32),
            pltpu.VMEM((size, 128), F32),
            pltpu.VMEM((leaves, slots, 3 * size), F32),
            pltpu.VMEM((leaves, slots, 128), F32),
            part,
            part,
            part,
            part,
            pltpu.VMEM((far_num * leaves, classes), BF16),
            pltpu.VMEM((far_num * leaves, cap * n), BF16),
            pltpu.VMEM((4, far_num * leaves, block), F32),
            pltpu.VMEM((far_num * leaves, period), F32),
            pltpu.VMEM((blocks * leaves, block), F32),
            pltpu.VMEM((block, 128), BF16),
            pltpu.VMEM((128, leaves * slots), BF16),
            pltpu.VMEM((cap * n, n * leaves), BF16),
            pltpu.VMEM((width, period), BF16),
            pltpu.VMEM((12, leaves, size), F32),
            pltpu.SemaphoreType.DMA((10,)),
            pltpu.SemaphoreType.DMA,
            pltpu.SemaphoreType.DMA((blocks,)),
            pltpu.SemaphoreType.DMA,
            pltpu.SemaphoreType.DMA((4,)),
            pltpu.SemaphoreType.DMA((4,)),
            pltpu.SemaphoreType.DMA((copies,)),
            pltpu.SemaphoreType.DMA((copies,)),
            pltpu.SemaphoreType.DMA((2,)),
            pltpu.SemaphoreType.DMA((2,)),
        ],
        compiler_params=pltpu.CompilerParams(
            collective_id=0,
            has_side_effects=True,
            vmem_limit_bytes=60 * 1024 * 1024,
        ),
    )(
        near_src.T,
        near_count,
        far_count,
        positions,
        densities,
        far_slot,
        far_class,
        requests[0].T,
        jnp.asarray(source_choice(), BF16),
        jnp.asarray(target_choice(size), BF16),
        up_basis,
        transfer_table,
        down,
    )


def solution(mesh):
    placed = (
        P(None, "patch"),
        P(None, "patch"),
        P("patch", None),
        P("patch"),
        P("patch", None),
        P("patch", None),
        P("patch"),
        P("patch", None, None),
        P("patch", None, None),
        P(),
        P("patch", None, None, None),
    )
    return jax.shard_map(
        functools.partial(per_device, mesh.shape["patch"]),
        mesh=mesh,
        in_specs=placed,
        out_specs=P(None, "patch"),
        check_vma=False,
    )
```

```python
import functools
import math

import jax
import jax.numpy as jnp
import numpy as np
from jax import lax
from jax.experimental import pallas as pl
from jax.experimental.pallas import tpu as pltpu
from jax.sharding import PartitionSpec as P

KERNEL = 1.0 / (8.0 * math.pi)
BLOB = 0.25
MESH = pl.DeviceIdType.MESH
F32 = jnp.float32
BF16 = jnp.bfloat16

ROWS = 48
FEATURES = 48
LEFT = (0, 0, 0, 1, 1, 2)
RIGHT = (0, 1, 2, 0, 1, 0)


def at(group):
    return (group // 2) * 8 + (group % 2) * 3


def source_choice():
    sel = np.zeros((4, FEATURES, ROWS), np.float32)
    for k in range(6):
        for c in range(3):
            sel[0, 3 * k + c, at(3 + RIGHT[k]) + c] = 1.0
            sel[1, 3 * k + c, at(6 + RIGHT[k]) + c] = -1.0
            sel[2, 18 + 3 * k + c, at(RIGHT[k]) + c] = 1.0
            sel[3, 18 + 3 * k + c, at(6 + RIGHT[k]) + c] = -2.0
    for c in range(3):
        sel[1, 36 + c, at(11) + c] = 1.0
        sel[2, 42 + c, at(9) + c] = -1.0
        sel[3, 39 + c, at(11) + c] = 1.0
        sel[3, 42 + c, at(10) + c] = 1.0
    return sel.reshape(4 * FEATURES, ROWS)


def target_choice(size):
    sel = np.zeros((ROWS, 128), np.float32)
    spread = np.zeros((ROWS, 6, size), np.float32)
    for k in range(6):
        for c in range(3):
            sel[at(LEFT[k]) + c, 3 * k + c] = 1.0
            sel[at(3 + LEFT[k]) + c, 18 + 3 * k + c] = 1.0
    for c in range(3):
        sel[at(6) + c, 36 + c] = 1.0
        sel[at(7) + c, 39 + c] = 1.0
        sel[at(8) + c, 42 + c] = 1.0
        for piece in range(3):
            spread[at(3 + piece) + c, c, :] = 3.0
            spread[at(piece) + c, 3 + c, :] = 1.0
    return np.concatenate([sel, spread.reshape(ROWS, 6 * size)], axis=1)


def iota(shape, dim):
    return lax.broadcasted_iota(jnp.int32, shape, dim)


def dot(a, b):
    return jnp.dot(a, b, preferred_element_type=F32)


def pieces(x):
    high = x.astype(BF16).astype(F32)
    rest = x - high
    mid = rest.astype(BF16).astype(F32)
    return high, mid, rest - mid


def inner(a, b):
    return a[0:1] * b[0:1] + a[1:2] * b[1:2] + a[2:3] * b[2:3]


def put(rows, group, value):
    rows[at(group) : at(group) + value.shape[0], : value.shape[1]] = value


def put_pieces(rows, group, value):
    for k, piece in enumerate(pieces(value)):
        if value.shape[0] == 3:
            put(rows, group + k, piece)
        else:
            rows[at(group) + k : at(group) + k + 1, : value.shape[1]] = piece


def source_rows(rows, x, f):
    put_pieces(rows, 0, f)
    put_pieces(rows, 3, f * (1.0 / 3.0))
    put_pieces(rows, 6, x)
    put_pieces(rows, 9, inner(f, x))
    put_pieces(rows, 10, inner(x, x) + BLOB)
    put(rows, 11, jnp.ones_like(x))


def target_rows(rows, x, f):
    a = f * KERNEL
    put_pieces(rows, 0, a)
    put_pieces(rows, 3, x)
    put_pieces(rows, 6, inner(a, x))
    put_pieces(rows, 7, inner(x, x))
    put(rows, 8, jnp.ones_like(x))


def flip(me, mask):
    bit = 1
    while bit <= mask:
        if mask & bit:
            me = me + bit - 2 * bit * lax.rem(lax.div(me, bit), 2)
        bit = 2 * bit
    return me


def split(n):
    bits = n.bit_length() - 1
    near = 1 << min(4, max(bits - 1, 0))
    return n // near, near


def body(
    n,
    near_src_hbm,
    near_count_hbm,
    far_count_hbm,
    pos_hbm,
    dens_hbm,
    far_slot_hbm,
    far_class_hbm,
    req_hbm,
    choose_src_hbm,
    choose_tgt_hbm,
    up_hbm,
    table_hbm,
    down_hbm,
    out,
    near_src,
    near_count,
    far_count,
    pos,
    dens,
    far_slot,
    far_class,
    req,
    choose_src,
    choose_tgt,
    pos_b,
    pos_a,
    dens_b,
    dens_a,
    up,
    table,
    down,
    dens_rows,
    mom,
    rows_own,
    rows_oth,
    window,
    rhs,
    lhs,
    tb,
    geo,
    tacc,
    cols,
    src_rows,
    hot_src,
    part_b,
    part_a,
    got_b,
    got_a,
    hot_class,
    hot_slot,
    ready,
    tiled,
    sums,
    fold,
    scatter,
    pick,
    spread,
    field,
    in_sem,
    up_sem,
    table_sem,
    down_sem,
    halo_send,
    halo_recv,
    mom_send,
    mom_recv,
    part_send,
    part_recv,
):
    leaves, width = mom.shape[1:]
    nodes = pos.shape[1]
    size = nodes // leaves
    slots = near_src.shape[0]
    far_num = far_slot.shape[1]
    classes = table.shape[0]
    cap = req.shape[0]
    block = fold.shape[0]
    outer, inner_n = split(n)
    expan_width = (width + 127) // 128 * 128
    me = lax.axis_index("patch")
    has_left = me > 0
    has_right = me < n - 1
    barrier = pltpu.get_barrier_semaphore()

    def signal(peer):
        pl.semaphore_signal(barrier, inc=1, device_id=(peer,), device_id_type=MESH)

    doublings = outer.bit_length() - 1
    for t in range(doublings):
        signal(flip(me, n >> (t + 1)))
    for k in range(1, inner_n):
        signal(flip(me, k))

    @pl.when(has_left)
    def _():
        signal(me - 1)

    @pl.when(has_right)
    def _():
        signal(me + 1)

    ins = [
        pltpu.make_async_copy(src, dst, in_sem.at[k])
        for k, (src, dst) in enumerate(
            (
                (pos_hbm, pos),
                (dens_hbm, dens),
                (choose_tgt_hbm, choose_tgt),
                (near_src_hbm, near_src),
                (near_count_hbm, near_count),
                (far_count_hbm, far_count),
                (far_slot_hbm, far_slot),
                (far_class_hbm, far_class),
                (req_hbm, req),
                (choose_src_hbm, choose_src),
            )
        )
    ]
    for copy in ins:
        copy.start()
    get_up = pltpu.make_async_copy(up_hbm, up, up_sem)
    get_up.start()

    def table_copy(b):
        lanes = pl.ds(pl.multiple_of(b * block, 128), block)
        return pltpu.make_async_copy(
            table_hbm.at[:, lanes], table.at[:, lanes], table_sem.at[b]
        )

    get_down = pltpu.make_async_copy(down_hbm, down, down_sem)
    for copy in ins:
        copy.wait()

    def halo(k, src, dst, peer):
        return pltpu.make_async_remote_copy(
            src_ref=src,
            dst_ref=dst,
            send_sem=halo_send.at[k],
            recv_sem=halo_recv.at[k],
            device_id=(peer,),
            device_id_type=MESH,
        )

    to_right = (halo(0, pos, pos_b, me + 1), halo(1, dens, dens_b, me + 1))
    to_left = (halo(2, pos, pos_a, me - 1), halo(3, dens, dens_a, me - 1))

    def gather(k, mask, first, count):
        return pltpu.make_async_remote_copy(
            src_ref=mom.at[0:count],
            dst_ref=mom.at[first : first + count],
            send_sem=mom_send.at[k],
            recv_sem=mom_recv.at[k],
            device_id=(flip(me, mask),),
            device_id_type=MESH,
        )

    far_step = [gather(t, n >> (t + 1), 1 << t, 1 << t) for t in range(doublings)]
    near_step = [
        gather(doublings - 1 + k, k, k * outer, outer) for k in range(1, inner_n)
    ]

    def sources(part, rows, x, f):
        source_rows(rows, x[...], f[...])
        for leaf in range(leaves):
            lanes = slice(leaf * size, (leaf + 1) * size)
            window[part * leaves + leaf, 0:3, :] = x[:, lanes] * 3.0
            window[part * leaves + leaf, 3:6, :] = f[:, lanes]

        for leaf in range(0, leaves, 2):
            chosen = dot(
                choose_src[...], rows[:, leaf * size : (leaf + 2) * size].astype(BF16)
            ).astype(BF16)
            for k in range(2):
                for o in range(4):
                    rhs[part * leaves + leaf + k, :, o * size : (o + 1) * size] = chosen[
                        o * FEATURES : (o + 1) * FEATURES, k * size : (k + 1) * size
                    ]

    rows_oth[...] = jnp.zeros_like(rows_oth)
    window[...] = jnp.zeros_like(window)
    nothing = jnp.zeros((3, size), F32)
    source_rows(rows_oth, nothing, nothing)
    chosen = dot(choose_src[...], rows_oth[:, :size].astype(BF16)).astype(BF16)
    for o in range(4):
        rhs[3 * leaves, :, o * size : (o + 1) * size] = chosen[
            o * FEATURES : (o + 1) * FEATURES
        ]
    sources(1, rows_oth, pos, dens)

    for leaf in range(leaves):
        for c in range(3):
            dens_rows[leaf : leaf + 1, c * size : (c + 1) * size] = dens[
                c : c + 1, leaf * size : (leaf + 1) * size
            ]
    dens_round = dens_rows[...].astype(BF16)
    get_up.wait()
    for b in range(width * width // block):
        table_copy(b).start()
    get_down.start()
    row = iota((leaves, width), 0)
    total = jnp.zeros((leaves, width), F32)
    for leaf in range(leaves):
        got = lax.dot_general(
            dens_round, up[leaf], (((1,), (1,)), ((), ())), preferred_element_type=F32
        )
        total = total + jnp.where(row == leaf, got, 0.0)
    mom[0] = total.astype(BF16)

    pl.semaphore_wait(
        barrier,
        doublings + inner_n - 1 + has_left.astype(jnp.int32) + has_right.astype(jnp.int32),
    )

    @pl.when(has_right)
    def _():
        for copy in to_right:
            copy.start()

    @pl.when(has_left)
    def _():
        for copy in to_left:
            copy.start()


    far_step[0].start()

    rows_own[...] = jnp.zeros_like(rows_own)
    target_rows(rows_own, pos[...], dens[...])

    few = 4

    for group in range(leaves // few):
        turned = []
        for k in range(few):
            start = pl.multiple_of((group * few + k) * size, size)
            turned.append(jnp.transpose(rows_own[:, pl.ds(start, size)]).astype(BF16))
        turned = jnp.concatenate(turned, axis=0)
        spread_out = dot(turned, choose_tgt[...])
        for k in range(few):
            mine = spread_out[k * size : (k + 1) * size]
            lhs[group * few + k] = mine[:, :128].astype(BF16)
            tb[group * few + k] = mine[:, 128:]

    count_col = jnp.zeros((leaves, 1), jnp.int32)
    leaf_col = iota((leaves, 1), 0)
    for leaf in range(leaves):
        count_col = jnp.where(leaf_col == leaf, far_count[leaf], count_col)
    class_iota = iota((leaves, classes), 1)
    column = iota((leaves, cap * n), 1)
    slot_of = lax.rem(column, n) * cap + lax.div(column, n)
    for s in range(far_num):
        rows = slice(s * leaves, (s + 1) * leaves)
        wanted = jnp.where(s < count_col, far_class[:, s : s + 1], -1)
        hot_class[rows, :] = (class_iota == wanted).astype(F32).astype(BF16)
        slot = far_slot[:, s : s + 1]
        hot_slot[rows, :] = (slot_of == slot).astype(F32).astype(BF16)
    fold_row = iota(fold.shape, 0)
    fold_first = iota(fold.shape, 1) * width
    fold[...] = (
        ((fold_row >= fold_first) & (fold_row < fold_first + width)).astype(F32).astype(BF16)
    )
    cols[...] = jnp.zeros_like(cols)
    offset = (me - 1) * leaves
    lane8 = iota((8, size), 1)
    lane1 = iota((1, 128), 1)

    def source_of(leaf, slot):
        live = slot < near_count[leaf]
        return jnp.where(live, near_src[slot, leaf] - offset, 3 * leaves)

    for leaf in range(leaves):
        for slot in range(slots):
            hot_src[leaf, slot : slot + 1, :] = (lane1 == source_of(leaf, slot)).astype(F32)
    scatter[...] = jnp.transpose(hot_src[...].reshape(leaves * slots, 128)).astype(BF16)

    device = iota((1, n), 1)
    place_of = jnp.zeros((1, n), jnp.int32)
    for t in range(n.bit_length() - 1):
        bit = 1 << t
        mine = lax.rem(lax.div(me, bit), 2)
        theirs = lax.rem(lax.div(device, bit), 2)
        place = bit * outer if bit < inner_n else n // (2 * bit)
        place_of = place_of + (theirs + mine - 2 * theirs * mine) * place
    row_iota = iota((n * leaves, n), 0)
    wanted = jnp.concatenate(
        [
            (row_iota == place_of * leaves + req[place : place + 1, :]).astype(F32)
            for place in range(cap)
        ],
        axis=1,
    )
    pick[...] = jnp.transpose(wanted).astype(BF16)
    period = tiled.shape[1]
    spread_gap = iota((width, period), 1) - iota((width, period), 0)
    near_gap = spread_gap == 0
    for k in range(1, period // width):
        near_gap = near_gap | (spread_gap == k * width)
    spread[...] = near_gap.astype(F32).astype(BF16)

    @pl.when(has_left)
    def _():
        for copy in to_right:
            copy.wait_recv()

    @pl.when(jnp.logical_not(has_left))
    def _():
        pos_b[...] = jnp.zeros_like(pos_b)
        dens_b[...] = jnp.zeros_like(dens_b)

    @pl.when(has_right)
    def _():
        for copy in to_left:
            copy.wait_recv()

    @pl.when(jnp.logical_not(has_right))
    def _():
        pos_a[...] = jnp.zeros_like(pos_a)
        dens_a[...] = jnp.zeros_like(dens_a)

    sources(0, rows_oth, pos_b, dens_b)
    sources(2, rows_own, pos_a, dens_a)

    together = 4
    ahead = 2
    halves = 1
    steps = together * slots
    turns = leaves // together

    def geometry(leaf, slot):
        return dot(lhs[leaf][:, :FEATURES], rhs[source_of(leaf, slot)])

    for k in range(ahead):
        geo[k][...] = geometry(0, k)

    step = 256 if block % 256 == 0 else 128
    per_block = block // width
    blocks = width * width // block
    early = ready.shape[0]
    share = early // turns
    jobs = [
        (k, t, h) for k in range(share) for t in range(block // step) for h in range(halves)
    ]

    def near_turn(turn):
        for k in range(share):
            table_copy(turn * share + k).wait()
        held = [geo[k] for k in range(ahead)]
        for sub in range(steps):
            leaf = turn * together + sub // slots
            slot = sub % slots
            nxt = sub + ahead
            if nxt < steps:
                held.append(geometry(turn * together + nxt // slots, nxt % slots))
            else:
                after = ((turn + 1) * together + (nxt - steps) // slots) % leaves
                geo[nxt - steps][...] = geometry(after, (nxt - steps) % slots)
            for job in range(sub * len(jobs) // steps, (sub + 1) * len(jobs) // steps):
                k, t, h = jobs[job]
                start = pl.multiple_of((turn * share + k) * block + t * step, 128)
                rows = far_num * leaves // halves
                lines = slice(h * rows, (h + 1) * rows)
                ready[turn * share + k, lines, t * step : (t + 1) * step] = dot(
                    hot_class[lines, :], table[:, pl.ds(start, step)]
                )
            now = held[sub]
            nodes_k = window[source_of(leaf, slot)]
            xs = [jnp.broadcast_to(nodes_k[c : c + 1], (8, size)) for c in range(3)]
            fs = [jnp.broadcast_to(nodes_k[3 + c : 4 + c], (8, size)) for c in range(3)]
            sums_src = [None] * 3
            for g in range(size // 8):
                r8 = slice(g * 8, (g + 1) * 8)
                ab, ar, br, rho = [now[r8, o * size : (o + 1) * size] for o in range(4)]
                inv1 = lax.rsqrt(rho)
                inv2 = inv1 * inv1
                inv3 = inv1 * inv2
                p = br * inv3
                q = ar * inv3
                w = ab * inv3 + (p * ar) * inv2
                for c in range(3):
                    sep = tb[leaf, r8, c * size : (c + 1) * size] - xs[c]
                    a = tb[leaf, r8, (3 + c) * size : (4 + c) * size]
                    term = a * p + fs[c] * q - w * sep
                    sums_src[c] = term if g == 0 else sums_src[c] + term
                    total = term if slot == 0 else term + tacc[c, r8, :]
                    if slot + 1 < slots:
                        tacc[c, r8, :] = total
                    else:
                        col = jnp.sum(total, axis=1, keepdims=True)
                        cols[r8, :] = jnp.where(lane8 == c * leaves + leaf, col, cols[r8, :])
            for c in range(3):
                src_rows[leaf, slot : slot + 1, c * size : (c + 1) * size] = jnp.sum(
                    sums_src[c], axis=0, keepdims=True
                )

    near_turn(0)
    for before, copy in zip(far_step, far_step[1:]):
        before.wait_recv()
        copy.start()
    far_step[-1].wait_recv()
    for copy in near_step:
        copy.start()

    @pl.loop(1, turns)
    def _(turn):
        near_turn(turn)

    for copy in near_step:
        copy.wait_recv()

    near_t = jnp.transpose(cols[...])
    values = src_rows[...].reshape(leaves * slots, 3 * size)
    scattered = None
    for piece in pieces(values):
        term = dot(scatter[...], piece.astype(BF16))
        scattered = term if scattered is None else scattered + term
    part_b[...] = scattered[:leaves]
    part_a[...] = scattered[2 * leaves : 3 * leaves]
    own = scattered[leaves : 2 * leaves]
    near = [
        near_t[c * leaves : (c + 1) * leaves] - own[:, c * size : (c + 1) * size]
        for c in range(3)
    ]
    for c in range(3):
        field[9 + c] = near[c]

    def part(k, src, dst, peer):
        return pltpu.make_async_remote_copy(
            src_ref=src,
            dst_ref=dst,
            send_sem=part_send.at[k],
            recv_sem=part_recv.at[k],
            device_id=(peer,),
            device_id_type=MESH,
        )

    part_left = part(0, part_b, got_a, me - 1)
    part_right = part(1, part_a, got_b, me + 1)

    @pl.when(has_left)
    def _():
        part_left.start()

    @pl.when(has_right)
    def _():
        part_right.start()

    moments = mom[...].reshape(n * leaves, width)
    chosen = dot(pick[...], moments).astype(BF16)
    chosen_rows = dot(chosen, spread[...]).astype(BF16)
    tiled[...] = dot(hot_slot[...], chosen_rows)


    def apply(members, t):
        for h in range(step // 128):
            tile = ((t * step) // 128 + h) % (period // 128)
            acc = [None] * len(members)
            for s in range(far_num):
                rows = slice(s * leaves, (s + 1) * leaves)
                factor = tiled[rows, tile * 128 : (tile + 1) * 128]
                for k, (b, oper) in enumerate(members):
                    term = oper(rows, h) * factor
                    acc[k] = term if acc[k] is None else acc[k] + term
            for k, (b, oper) in enumerate(members):
                lines = pl.ds(pl.multiple_of(b * leaves, leaves), leaves)
                sums[lines, t * step + h * 128 : t * step + (h + 1) * 128] = acc[k]

    def fresh(b, t):
        start = pl.multiple_of(b * block + t * step, 128)
        oper = dot(hot_class[...], table[:, pl.ds(start, step)])
        return b, lambda rows, h: oper[rows, h * 128 : (h + 1) * 128]

    def stored(b, t):
        return b, lambda rows, h: ready[
            b, rows, t * step + h * 128 : t * step + (h + 1) * 128
        ]

    paired = min(early, blocks - early)

    @pl.loop(0, paired // 2)
    def _(turn):
        for k in range(2):
            table_copy(early + turn * 2 + k).wait()
        for k in range(2):
            b = turn * 2 + k
            for t in range(block // step):
                apply((fresh(early + b, t), stored(b, t)), t)

    for b in range(early + paired, blocks):
        table_copy(b).wait()
        for t in range(block // step):
            apply((fresh(b, t),), t)

    whole = sums[...]
    high = whole.astype(BF16)
    low = (whole - high.astype(F32)).astype(BF16)
    res = dot(high, fold[...]) + dot(low, fold[...])
    wide = jnp.zeros((leaves, expan_width), F32)
    for b in range(blocks):
        one = jnp.concatenate(
            [res[b * leaves : (b + 1) * leaves], jnp.zeros((leaves, expan_width - 128), F32)], axis=1
        )
        wide = wide + (pltpu.roll(one, b * per_block, 1) if b else one)
    expansion = wide[:, :width]
    get_down.wait()
    leaf_row = iota((leaves, width), 0)
    nothing = jnp.zeros_like(expansion)
    single = [
        jnp.where(leaf_row == leaf, expansion, nothing).astype(BF16) for leaf in range(leaves)
    ]
    on_vpu = 3
    for q in range(9 - on_vpu):
        total = None
        for leaf in range(leaves):
            got = dot(single[leaf], down[leaf, q])
            total = got if total is None else total + got
        field[q] = total
    padded = jnp.concatenate([wide, jnp.zeros((128 - leaves, expan_width), F32)], axis=0)
    turned = jnp.transpose(padded.astype(BF16).astype(F32))[:width]
    for leaf in range(leaves):
        column = jnp.broadcast_to(turned[:, leaf : leaf + 1], (width, size))
        for q in range(9 - on_vpu, 9):
            product = column * down[leaf, q].astype(F32)
            field[q, leaf : leaf + 1, :] = jnp.sum(product, axis=0, keepdims=True)

    @pl.when(has_right)
    def _():
        part_left.wait_recv()

    @pl.when(jnp.logical_not(has_right))
    def _():
        got_a[...] = jnp.zeros_like(got_a)

    @pl.when(has_left)
    def _():
        part_right.wait_recv()

    @pl.when(jnp.logical_not(has_left))
    def _():
        got_b[...] = jnp.zeros_like(got_b)

    for k in range(3):
        lanes = slice(k * size, (k + 1) * size)
        result = field[9 + k] - (got_b[:, lanes] + got_a[:, lanes])
        for c in range(3):
            result = result + dens_rows[:, c * size : (c + 1) * size] * field[3 * c + k]
        for leaf in range(leaves):
            out[k : k + 1, leaf * size : (leaf + 1) * size] = result[leaf : leaf + 1]

    @pl.when(has_right)
    def _():
        part_right.wait_send()
        for copy in to_right:
            copy.wait_send()

    @pl.when(has_left)
    def _():
        part_left.wait_send()
        for copy in to_left:
            copy.wait_send()

    for copy in far_step + near_step:
        copy.wait_send()


def per_device(
    n,
    positions,
    densities,
    near_src,
    near_count,
    far_slot,
    far_class,
    far_count,
    requests,
    up_basis,
    transfer_table,
    down_basis,
):
    leaves, slots = near_src.shape
    nodes = positions.shape[1]
    size = nodes // leaves
    width = up_basis.shape[1]
    far_num = far_slot.shape[1]
    cap = requests.shape[2]
    classes = transfer_table.shape[0]
    copies = split(n)[0].bit_length() + split(n)[1] - 2
    period = math.lcm(width, 128)
    blocks = width * width // period
    block = 2 * period if blocks % 2 == 0 else period
    down = jnp.transpose(down_basis, (0, 2, 1, 3))
    blocks = width * width // block
    vmem = pl.BlockSpec(memory_space=pltpu.VMEM)
    hbm = pl.BlockSpec(memory_space=pl.ANY)
    line = pltpu.VMEM((3, nodes), F32)
    part = pltpu.VMEM((leaves, 3 * size), F32)
    return pl.pallas_call(
        functools.partial(body, n),
        out_shape=pltpu.VMEM((3, nodes), F32),
        in_specs=[hbm] * 13,
        out_specs=vmem,
        scratch_shapes=[
            pltpu.SMEM((slots, leaves), jnp.int32),
            pltpu.SMEM((leaves,), jnp.int32),
            pltpu.SMEM((leaves,), jnp.int32),
            line,
            line,
            pltpu.VMEM(far_slot.shape, jnp.int32),
            pltpu.VMEM(far_class.shape, jnp.int32),
            pltpu.VMEM((cap, n), jnp.int32),
            pltpu.VMEM((4 * FEATURES, ROWS), BF16),
            pltpu.VMEM((ROWS, 128 + 6 * size), BF16),
        ]
        + [line] * 4
        + [
            pltpu.VMEM(up_basis.shape, BF16),
            pltpu.VMEM(transfer_table.shape, BF16),
            pltpu.VMEM(down.shape, BF16),
            part,
            pltpu.VMEM((n, leaves, width), BF16),
            pltpu.VMEM((ROWS, nodes), F32),
            pltpu.VMEM((ROWS, nodes), F32),
            pltpu.VMEM((3 * leaves + 1, 8, size), F32),
            pltpu.VMEM((3 * leaves + 1, FEATURES, 4 * size), BF16),
            pltpu.VMEM((leaves, size, 128), BF16),
            pltpu.VMEM((leaves, size, 6 * size), F32),
            [pltpu.VMEM((size, 4 * size), F32)] * 2,
            pltpu.VMEM((3, size, size), F32),
            pltpu.VMEM((size, 128), F32),
            pltpu.VMEM((leaves, slots, 3 * size), F32),
            pltpu.VMEM((leaves, slots, 128), F32),
            part,
            part,
            part,
            part,
            pltpu.VMEM((far_num * leaves, classes), BF16),
            pltpu.VMEM((far_num * leaves, cap * n), BF16),
            pltpu.VMEM((4, far_num * leaves, block), F32),
            pltpu.VMEM((far_num * leaves, period), F32),
            pltpu.VMEM((blocks * leaves, block), F32),
            pltpu.VMEM((block, 128), BF16),
            pltpu.VMEM((128, leaves * slots), BF16),
            pltpu.VMEM((cap * n, n * leaves), BF16),
            pltpu.VMEM((width, period), BF16),
            pltpu.VMEM((12, leaves, size), F32),
            pltpu.SemaphoreType.DMA((10,)),
            pltpu.SemaphoreType.DMA,
            pltpu.SemaphoreType.DMA((blocks,)),
            pltpu.SemaphoreType.DMA,
            pltpu.SemaphoreType.DMA((4,)),
            pltpu.SemaphoreType.DMA((4,)),
            pltpu.SemaphoreType.DMA((copies,)),
            pltpu.SemaphoreType.DMA((copies,)),
            pltpu.SemaphoreType.DMA((2,)),
            pltpu.SemaphoreType.DMA((2,)),
        ],
        compiler_params=pltpu.CompilerParams(
            collective_id=0,
            has_side_effects=True,
            vmem_limit_bytes=60 * 1024 * 1024,
        ),
    )(
        near_src.T,
        near_count,
        far_count,
        positions,
        densities,
        far_slot,
        far_class,
        requests[0].T,
        jnp.asarray(source_choice(), BF16),
        jnp.asarray(target_choice(size), BF16),
        up_basis,
        transfer_table,
        down,
    )


def solution(mesh):
    placed = (
        P(None, "patch"),
        P(None, "patch"),
        P("patch", None),
        P("patch"),
        P("patch", None),
        P("patch", None),
        P("patch"),
        P("patch", None, None),
        P("patch", None, None),
        P(),
        P("patch", None, None, None),
    )
    return jax.shard_map(
        functools.partial(per_device, mesh.shape["patch"]),
        mesh=mesh,
        in_specs=placed,
        out_specs=P(None, "patch"),
        check_vma=False,
    )
```
